32 devices in a mesh: row: 8 (over y, x, core), col: 4 (over z).
Axes of the slice: x: 2, y: 2, z: 4, core: 2. Of those that a mesh axis runs over, the one named last changes fastest.
Arguments:
- tokens: bfloat16 [6144, 2048], P('row', 'col'), may hold values from -6 to 6
- out_grad: bfloat16 [6144, 2048], P('row', 'col'), may hold values from -768 to 768
- counts: int32 [8], P('row'), may hold values from 65 to 768
- block_moves: int32 [4, 3], replicated, may hold values from 0 to 7, as said below
- segment_ids: int32 [6144], P('row'), may hold values from 0 to 191, never falling along the last dimension, each value on 1 to 128 neighbouring positions
- gate_weight: bfloat16 [2048, 8192], P('row', 'col'), may hold values from -0.125 to 0.125
- up_weight: bfloat16 [2048, 8192], P('row', 'col'), may hold values from -0.125 to 0.125
- down_weight: bfloat16 [2048, 8192], P('row', 'col'), may hold values from -0.0625 to 0.0625
Outputs:
- hidden: bfloat16 [4096, 8192], P('row', 'col')
- gate_grad: float32 [2048, 8192], P('row', 'col')
- up_grad: float32 [2048, 8192], P('row', 'col')
- down_grad: float32 [2048, 8192], P('row', 'col')
The draws below stay inside these ranges and needn't reach their ends.
Inputs may be any that keep to these rules, and one draw needn't show every extreme that they name: `block_moves`: each row is (source rank, destination rank, block index); the block is a valid block of its source; no two rows share both source and destination, nor both source and block; a rank is the source of at most two rows or the destination of at most one, never both; after the moves every rank holds at most 4 valid blocks and some hold exactly 4. `segment_ids`: never falling along the whole array; each document covers 1 to 128 consecutive slots.
All inputs are finite; a program needn't handle non-finite values.
Results may differ from the reference program's by a relative error of at most 0.015.
Values may be sent and summed in bfloat16 or wider, within the bound.
A program may use at most 128 MiB of HBM per device.

```python
import math
import jax
import jax.numpy as jnp
import numpy as np
from jax import lax

D = 2048
F = 8192
BLOCK = 128
WORK = 4
CAP = 6
TOK_DEV = 768
TOKENS = 6144
MOVES = 4
N_ROW = 8


def rebalance_plan(key):
    perm_key, light_key, part_key, pick_key, flip_key = jax.random.split(key, 5)
    groups = N_ROW // 4
    half = N_ROW // 2
    pair_order = jax.random.permutation(perm_key, half).astype(jnp.int32).reshape(groups, 2)
    flips = jax.random.randint(flip_key, (groups, 2), 0, 2, dtype=jnp.int32)
    low_rank = pair_order
    high_rank = pair_order + half
    first_rank = jnp.where(flips == 0, low_rank, high_rank)
    second_rank = jnp.where(flips == 0, high_rank, low_rank)
    order_ranks = jnp.stack([first_rank[:, 0], second_rank[:, 0], first_rank[:, 1], second_rank[:, 1]], axis=1).astype(jnp.int32)
    spare_load = jax.random.randint(light_key, (groups,), 1, WORK + 1, dtype=jnp.int32)
    heavy_load = jnp.full((groups,), WORK + 2, jnp.int32)
    lean_load = jnp.full((groups,), WORK - 1, jnp.int32)
    all_loads = jnp.stack([heavy_load, lean_load, lean_load, spare_load], axis=1).reshape(-1)
    block_counts = jnp.zeros((N_ROW,), jnp.int32).at[order_ranks.reshape(-1)].set(all_loads)
    tail_fill = jax.random.randint(part_key, (N_ROW,), BLOCK // 2 + 1, BLOCK + 1, dtype=jnp.int32)
    counts = ((block_counts - 1) * BLOCK + tail_fill).astype(jnp.int32)
    chosen = jax.vmap(lambda sub_key: jax.random.permutation(sub_key, WORK + 2)[:2])(jax.random.split(pick_key, groups)).astype(jnp.int32)
    first_move = jnp.stack([order_ranks[:, 0], order_ranks[:, 1], chosen[:, 0]], axis=1)
    second_move = jnp.stack([order_ranks[:, 0], order_ranks[:, 2], chosen[:, 1]], axis=1)
    block_moves = jnp.stack([first_move, second_move], axis=1).reshape(N_ROW // 2, 3).astype(jnp.int32)
    return (counts, block_moves)


def draw_counts(key, part):
    return rebalance_plan(jax.random.fold_in(key, 11))[0]


def draw_block_moves(key, part):
    return rebalance_plan(jax.random.fold_in(key, 11))[1]


def level_of(key, extent, cuts, smallest, largest):
    loudness, own = 1.0, jax.random.fold_in(key, 6)
    for dim, shards_of in cuts:
        steps = jnp.exp(jax.random.uniform(jax.random.fold_in(own, dim), (shards_of,), jnp.float32, smallest / len(cuts), largest / len(cuts)))
        loudness = loudness * jnp.repeat(steps, extent[dim] // shards_of).reshape([-1 if axis == dim else 1 for axis in range(len(extent))])
    return loudness


def length_profile(number_of, total, reach, slope):
    loads = [(1 << 20) // math.isqrt(rank ** slope) + 1 for rank in range(2, number_of + 1)]
    surplus, given = total - reach - (number_of - 1), [1] * (number_of - 1)
    while surplus > 0:
        candidates = [i for i in range(number_of - 1) if given[i] < reach]
        mass, left = sum([loads[i] for i in candidates]), surplus
        for i in candidates:
            extra = min(reach - given[i], max(1, left * loads[i] // mass), surplus)
            given[i] = given[i] + extra
            surplus = surplus - extra
    return np.array([reach] + given)


def uneven_parts(rng, number_of, total, most, lean):
    if number_of == 2:
        one = jax.random.randint(rng, (), max(1, total - most), min(most, total - 1) + 1)
        return jnp.stack([one, total - one])
    sizes = jnp.asarray(length_profile(number_of, total, most, lean), jnp.int32)
    twos = (number_of - 1) // 2
    source_of, sink = sizes[1:1 + 2 * twos:2], sizes[2:2 + 2 * twos:2]
    slack = jnp.minimum(source_of - 1, most - sink)
    passed = jax.random.randint(jax.random.fold_in(rng, 1), (twos,), 0, 1 << 20) % (slack + 1)
    sizes = sizes.at[1:1 + 2 * twos:2].set(source_of - passed).at[2:2 + 2 * twos:2].set(sink + passed)
    return sizes[jax.random.permutation(jax.random.fold_in(rng, 2), number_of)]


def scatter_about(rng, extent, spread, limit, cuts=(), held_as=jnp.bfloat16):
    result = jax.random.normal(rng, extent, jnp.float32) * spread
    if len(cuts) > 0:
        result = level_of(rng, extent, cuts, -0.22, 0.18) * result
    return jnp.clip(result, min=-limit, max=limit).astype(held_as)


def setup_inputs(seed: int = 0) -> dict:
    splits = jax.random.split(jax.random.key(seed), 9)
    return {
        "tokens": scatter_about(splits[0], (TOKENS, D), 1.0, 6.0, ((0, 8), (1, 4))),
        "out_grad": scatter_about(splits[1], (TOKENS, D), (16 * N_ROW), 768.0, ((0, 8), (1, 4))),
        "counts": draw_counts(jax.random.fold_in(splits[8], 71), 0),
        "block_moves": draw_block_moves(jax.random.fold_in(splits[8], 71), 0),
        "segment_ids": jnp.searchsorted(jnp.cumsum(uneven_parts(splits[4], TOKENS // 32, TOKENS, 128, 2)), jnp.arange(TOKENS), side="right").astype(jnp.int32),
        "gate_weight": scatter_about(splits[5], (D, F), D ** -0.5, 0.125, ((0, 8), (1, 4))),
        "up_weight": scatter_about(splits[6], (D, F), D ** -0.5, 0.125, ((0, 8), (1, 4))),
        "down_weight": scatter_about(splits[7], (D, F), F ** -0.5, 0.0625, ((0, 8), (1, 4))),
    }


def loss_mask(counts, segment_ids):
    segments = segment_ids.reshape(N_ROW, TOK_DEV)
    following = jnp.concatenate([segments[:, 1:], segments[:, -1:]], axis=1)
    places = jnp.arange(TOK_DEV, dtype=jnp.int32)[None, :]
    kept_flag = (places + 1 < counts[:, None]) & (following == segments)
    return kept_flag.astype(jnp.float32)


def work_index(counts, block_moves):
    source = block_moves[:, 0]
    target = block_moves[:, 1]
    block_id = block_moves[:, 2]
    rank_ids = jnp.arange(N_ROW, dtype=jnp.int32)
    block_ids = jnp.arange(CAP, dtype=jnp.int32)
    filled = (counts + BLOCK - 1) // BLOCK
    moved_out = jnp.any((source[None, None, :] == rank_ids[:, None, None]) & (block_id[None, None, :] == block_ids[None, :, None]), axis=2)
    kept_flag = (block_ids[None, :] < filled[:, None]) & jnp.logical_not(moved_out)
    arrive = target[None, :] == rank_ids[:, None]
    flag_bits = jnp.concatenate([kept_flag, arrive], axis=1).astype(jnp.int32)
    own_ids = (rank_ids[:, None] * CAP + block_ids[None, :]).astype(jnp.int32)
    came_ids = jnp.broadcast_to((source * CAP + block_id)[None, :], (N_ROW, MOVES)).astype(jnp.int32)
    source_ids = jnp.concatenate([own_ids, came_ids], axis=1)
    list_place = (jnp.cumsum(flag_bits, axis=1) - 1).astype(jnp.int32)
    slot_ids = jnp.arange(WORK, dtype=jnp.int32)
    slot_hit = (flag_bits[:, :, None] == 1) & (list_place[:, :, None] == slot_ids[None, None, :])
    chosen = jnp.sum(jnp.where(slot_hit, source_ids[:, :, None] + 1, 0), axis=1).astype(jnp.int32)
    return (chosen - 1).astype(jnp.int32)


def pick_blocks(block_rows, slot_index):
    flat_index = slot_index.reshape(-1)
    picked = jnp.take(block_rows, jnp.maximum(flat_index, 0), axis=0)
    live_rows = (flat_index >= 0).reshape((-1,) + (1,) * (picked.ndim - 1))
    return jnp.where(live_rows, picked, jnp.zeros_like(picked))


def local_terms(gate_sum, up_sum, back_sum):
    logistic = jax.nn.sigmoid(gate_sum)
    activated = gate_sum * logistic
    hidden = (activated * up_sum).astype(jnp.bfloat16)
    gate_back = (back_sum * up_sum * logistic * (1.0 + gate_sum * (1.0 - logistic))).astype(jnp.bfloat16)
    up_back = (back_sum * activated).astype(jnp.bfloat16)
    return hidden, gate_back, up_back


def contract(left_side, right_side):
    return lax.dot_general(left_side, right_side, (((0,), (0,)), ((), ())), preferred_element_type=jnp.float32)


def reference(tokens, out_grad, counts, block_moves, segment_ids, gate_weight, up_weight, down_weight):
    weight_mask = loss_mask(counts, segment_ids)
    loss_total = jnp.sum(weight_mask)
    slot_index = work_index(counts, block_moves)
    work_tokens = pick_blocks(tokens.reshape(N_ROW * CAP, BLOCK, D), slot_index).reshape(N_ROW, WORK * BLOCK, D)
    work_grad = pick_blocks(out_grad.reshape(N_ROW * CAP, BLOCK, D), slot_index).reshape(N_ROW, WORK * BLOCK, D)
    work_weight = pick_blocks(weight_mask.reshape(N_ROW * CAP, BLOCK), slot_index).reshape(N_ROW, WORK * BLOCK)

    def per_rank(running, inputs):
        tok_rows, grad_rows, row_weight = inputs
        gate_sum = jnp.dot(tok_rows, gate_weight, preferred_element_type=jnp.float32)
        up_sum = jnp.dot(tok_rows, up_weight, preferred_element_type=jnp.float32)
        back_sum = jnp.dot(grad_rows, down_weight, preferred_element_type=jnp.float32) * row_weight[:, None]
        hidden, gate_back, up_back = local_terms(gate_sum, up_sum, back_sum)
        weighted = grad_rows * row_weight.astype(jnp.bfloat16)[:, None]
        new_terms = (contract(tok_rows, gate_back), contract(tok_rows, up_back), contract(weighted, hidden))
        rounded = tuple(lax.optimization_barrier((term_sum / loss_total).astype(jnp.bfloat16)).astype(jnp.float32) for term_sum in new_terms)
        return tuple(total_part + new_part for total_part, new_part in zip(running, rounded)), hidden

    zero_sums = jnp.zeros((D, F), jnp.float32)
    grad_sums, hidden_all = lax.scan(per_rank, (zero_sums, zero_sums, zero_sums), (work_tokens, work_grad, work_weight))
    return hidden_all.reshape(N_ROW * WORK * BLOCK, F), grad_sums[0], grad_sums[1], grad_sums[2]
```

```python
import functools

import jax
import jax.numpy as jnp
from jax import lax
from jax.experimental import pallas as pl
from jax.experimental.pallas import tpu as pltpu
from jax.sharding import PartitionSpec as P

BLOCK = 128
WORK = 4
MESH = pl.DeviceIdType.MESH


def local_terms(gate_sum, up_sum, back_sum):
    logistic = jax.nn.sigmoid(gate_sum)
    activated = gate_sum * logistic
    hidden = (activated * up_sum).astype(jnp.bfloat16)
    gate_back = (back_sum * up_sum * logistic * (1.0 + gate_sum * (1.0 - logistic))).astype(
        jnp.bfloat16
    )
    up_back = (back_sum * activated).astype(jnp.bfloat16)
    return (hidden, gate_back, up_back)


def contract(left_side, right_side):
    return lax.dot_general(
        left_side, right_side, (((0,), (0,)), ((), ())), preferred_element_type=jnp.float32
    )


def ring_gather(piece):
    ranks = lax.axis_size("col")
    me = lax.axis_index("col")
    rows, cols = piece.shape
    shift = [(i, (i + 1) % ranks) for i in range(ranks)]
    whole = jnp.zeros((rows, ranks * cols), piece.dtype)
    whole = lax.dynamic_update_slice(whole, piece, (0, me * cols))
    for step in range(1, ranks):
        piece = lax.ppermute(piece, "col", shift)
        owner = (me - step + ranks) % ranks
        whole = lax.dynamic_update_slice(whole, piece, (0, owner * cols))
    return whole


def plain_device(
    tokens, out_grad, counts, block_moves, segment_ids, gate_weight, up_weight, down_weight
):
    ranks_all = lax.axis_size("row")
    me_rank = lax.axis_index("row")
    slot_rows = tokens.shape[0]
    cap_blocks = slot_rows // BLOCK
    feat_cols = tokens.shape[1]
    my_count = counts[0]
    places = jnp.arange(slot_rows, dtype=jnp.int32)
    following = jnp.concatenate([segment_ids[1:], segment_ids[-1:]])
    own_weight = ((places + 1 < my_count) & (following == segment_ids)).astype(jnp.float32)
    source = block_moves[:, 0]
    target = block_moves[:, 1]
    block_id = block_moves[:, 2]
    block_ids = jnp.arange(cap_blocks, dtype=jnp.int32)
    filled = (my_count + BLOCK - 1) // BLOCK
    moved_out = jnp.any(
        (source[None, :] == me_rank) & (block_id[None, :] == block_ids[:, None]), axis=1
    )
    kept_flag = (block_ids < filled) & jnp.logical_not(moved_out)
    arrive = target == me_rank
    flag_bits = jnp.concatenate([kept_flag, arrive]).astype(jnp.int32)
    local_ids = jnp.concatenate([block_ids, cap_blocks + source])
    list_place = jnp.cumsum(flag_bits) - 1
    slot_ids = jnp.arange(WORK, dtype=jnp.int32)
    slot_hit = (flag_bits[:, None] == 1) & (list_place[:, None] == slot_ids[None, :])
    slot_index = jnp.sum(jnp.where(slot_hit, local_ids[:, None] + 1, 0), axis=0) - 1
    peer_ids = jnp.arange(ranks_all, dtype=jnp.int32)
    outgoing = (source[None, :] == me_rank) & (target[None, :] == peer_ids[:, None])
    send_block = jnp.sum(jnp.where(outgoing, block_id[None, :], 0), axis=1)
    send_live = jnp.any(outgoing, axis=1)
    own_both = jnp.concatenate([tokens, out_grad], axis=1).reshape(cap_blocks, BLOCK, 2 * feat_cols)
    own_mask = own_weight.astype(jnp.bfloat16).reshape(cap_blocks, BLOCK)

    def outbox(block_rows):
        chosen = jnp.take(block_rows, send_block, axis=0)
        live_rows = send_live.reshape((-1,) + (1,) * (chosen.ndim - 1))
        return jnp.where(live_rows, chosen, jnp.zeros_like(chosen))

    whole_count = jnp.sum(own_weight).astype(jnp.int32)
    count_parts = jnp.broadcast_to(
        jnp.stack([whole_count // 256, whole_count % 256]).astype(jnp.bfloat16)[None, :],
        (ranks_all, 2),
    )
    got_both = lax.all_to_all(outbox(own_both), "row", split_axis=0, concat_axis=0, tiled=True)
    got_small = lax.all_to_all(
        jnp.concatenate([outbox(own_mask), count_parts], axis=1),
        "row",
        split_axis=0,
        concat_axis=0,
        tiled=True,
    )
    got_mask = got_small[:, :BLOCK]
    part_values = got_small[:, BLOCK:].astype(jnp.float32)
    loss_total = 256.0 * jnp.sum(part_values[:, 0]) + jnp.sum(part_values[:, 1])

    def to_work(pool_rows):
        chosen = jnp.take(pool_rows, jnp.maximum(slot_index, 0), axis=0)
        live_rows = (slot_index >= 0).reshape((-1,) + (1,) * (chosen.ndim - 1))
        return jnp.where(live_rows, chosen, jnp.zeros_like(chosen))

    work_both = to_work(jnp.concatenate([own_both, got_both])).reshape(WORK * BLOCK, 2 * feat_cols)
    work_mask = to_work(jnp.concatenate([own_mask, got_mask])).reshape(WORK * BLOCK)
    work_weight = work_mask.astype(jnp.float32)
    hidden_cols = gate_weight.shape[1]
    token_piece = work_both[:, :feat_cols]
    grad_piece = work_both[:, feat_cols:]
    full_tokens = ring_gather(token_piece)
    full_grad = ring_gather(grad_piece)
    gate_piece = lax.all_gather(gate_weight, "row", axis=0, tiled=True)
    up_piece = lax.all_gather(up_weight, "row", axis=0, tiled=True)
    down_piece = lax.all_gather(down_weight, "row", axis=0, tiled=True)
    gate_sum = jnp.dot(full_tokens, gate_piece, preferred_element_type=jnp.float32)
    up_sum = jnp.dot(full_tokens, up_piece, preferred_element_type=jnp.float32)
    back_raw = jnp.dot(full_grad, down_piece, preferred_element_type=jnp.float32)
    back_sum = back_raw * work_weight[:, None]
    hidden, gate_back, up_back = local_terms(gate_sum, up_sum, back_sum)
    weighted = full_grad * work_mask[:, None]

    def term_rows(left_side, right_side):
        return contract(left_side, right_side) / loss_total

    down_grad = lax.psum_scatter(
        term_rows(weighted, hidden).astype(jnp.bfloat16), "row", scatter_dimension=0, tiled=True
    ).astype(jnp.float32)
    other_part = lax.psum_scatter(
        jnp.concatenate(
            [term_rows(full_tokens, gate_back), term_rows(full_tokens, up_back)], axis=1
        ).astype(jnp.bfloat16),
        "row",
        scatter_dimension=0,
        tiled=True,
    ).astype(jnp.float32)
    gate_grad = other_part[:, :hidden_cols]
    up_grad = other_part[:, hidden_cols:]
    return (hidden, gate_grad, up_grad, down_grad)


EARLY, LATE = 0, 1


def contract_rows(left_side, right_side):
    return lax.dot_general(
        left_side, right_side, (((0,), (0,)), ((), ())), preferred_element_type=jnp.float32
    )


def grouped_kernel(
    ranks,
    cols,
    cap,
    count_ref,
    moves_ref,
    tok_ref,
    grad_ref,
    mine_ref,
    gate_ref,
    up_ref,
    down_ref,
    hid_ref,
    sum_ref,
    total_ref,
    own,
    every,
    weights,
    hid,
    backs,
    outbox,
    carry,
    came,
    leave,
    enter,
    part,
    final,
    tallies,
    r_unit,
    s_x,
    s_up,
    s_dn,
    s_sib,
    r_w,
    s_w,
    s_loc,
    r_box,
    s_box,
    s_carry,
    r_carry,
    s_tally,
    r_tally,
    s_leave,
    r_leave,
    s_final,
    r_final,
    s_hid,
    r_hid,
):
    group = ranks // 2
    r = lax.axis_index("row")
    c = lax.axis_index("col")
    y = r // group
    q = r % group
    x = q // 2
    k = q % 2
    q_sib = x * 2 + 1 - k
    q_x = (1 - x) * 2 + k
    q_d = (1 - x) * 2 + 1 - k
    base = y * group
    far = (1 - y) * group
    wide = own.shape[2]
    drow = gate_ref.shape[0]
    fcol = weights.shape[2]
    early_rows = (WORK - 1) * BLOCK
    late_base = group * early_rows

    def at(row):
        return (row, c)

    barrier = pltpu.get_barrier_semaphore()
    for step in range(1, ranks):
        pl.semaphore_signal(
            barrier, inc=1, device_id=at(lax.rem(r + step, ranks)), device_id_type=MESH
        )

    @pl.when(c + 1 < cols)
    def _():
        pl.semaphore_signal(barrier, inc=1, device_id=(r, c + 1), device_id_type=MESH)

    @pl.when(c > 0)
    def _():
        pl.semaphore_signal(barrier, inc=1, device_id=(r, c - 1), device_id_type=MESH)

    moves = moves_ref.shape[0]
    src = [moves_ref[m, 0] for m in range(moves)]
    dst = [moves_ref[m, 1] for m in range(moves)]
    blk = [moves_ref[m, 2] for m in range(moves)]

    def as_int(flag):
        return jnp.where(flag, 1, 0)

    order = []
    for m in range(moves):
        before = jnp.int32(0)
        for e in range(m):
            before = before + as_int(src[e] == src[m])
        order.append(before)
    filled = (count_ref[0] + BLOCK - 1) // BLOCK
    slot_id = [jnp.int32(0)] * WORK
    slot_ok = [jnp.int32(0)] * WORK
    held = jnp.int32(0)
    for b in range(cap):
        gone = jnp.int32(0)
        for m in range(moves):
            gone = gone + as_int((src[m] == r) & (blk[m] == b))
        keep = as_int((b < filled) & (gone == 0))
        for s in range(WORK):
            hit = keep * as_int(held == s)
            slot_id[s] = slot_id[s] + b * hit
            slot_ok[s] = slot_ok[s] + hit
        held = held + keep
    box_id = [jnp.int32(0), jnp.int32(0)]
    box_ok = [jnp.int32(0), jnp.int32(0)]
    near_id = jnp.int32(0)
    near_ok = jnp.int32(0)
    far_ok = jnp.int32(0)
    pass_id = jnp.int32(0)
    pass_ok = jnp.int32(0)
    for m in range(moves):
        for j in range(2):
            hit = as_int((src[m] == r) & (order[m] == j))
            box_id[j] = box_id[j] + blk[m] * hit
            box_ok[j] = box_ok[j] + hit
        inside = as_int(src[m] // group == y)
        place = (src[m] % group) * 2 + order[m]
        mine = as_int(dst[m] == r)
        near_id = near_id + mine * inside * place
        near_ok = near_ok + mine * inside
        far_ok = far_ok + mine * (1 - inside)
        over = as_int(dst[m] == far + q) * inside
        pass_id = pass_id + over * place
        pass_ok = pass_ok + over

    def kept(ref, index, ok):
        value = ref[index]
        return jnp.where(ok > 0, value, jnp.zeros_like(value))

    for j in range(2):
        outbox[q * 2 + j, 0] = kept(tok_ref, box_id[j], box_ok[j])
        outbox[q * 2 + j, 1] = kept(grad_ref, box_id[j], box_ok[j])

    my_cols = pl.ds(pl.multiple_of(c * wide, wide), wide)
    for s in range(WORK - 1):
        rows = pl.ds(pl.multiple_of(q * early_rows + s * BLOCK, BLOCK), BLOCK)
        for which, ref in enumerate((tok_ref, grad_ref)):
            value = kept(ref, slot_id[s], slot_ok[s])
            own[which, s * BLOCK : (s + 1) * BLOCK] = value
            every[which, rows, my_cols] = value

    sends = []

    def remote(source, target, send_sem, recv_sem, device, when=None):
        copy = pltpu.make_async_remote_copy(
            src_ref=source,
            dst_ref=target,
            send_sem=send_sem,
            recv_sem=recv_sem,
            device_id=device,
            device_id_type=MESH,
        )
        sends.append((when, copy))
        if when is None:
            copy.start()
        else:
            pl.when(when)(lambda: copy.start())

    def arrival(target, recv_sem, when=None):
        copy = pltpu.make_async_remote_copy(
            src_ref=target,
            dst_ref=target,
            send_sem=s_tally.at[0],
            recv_sem=recv_sem,
            device_id=at(r),
            device_id_type=MESH,
        )
        if when is None:
            copy.wait_recv()
        else:
            pl.when(when)(lambda: copy.wait_recv())

    size = (early_rows, BLOCK)

    def unit(stage, owner, column):
        start = owner * size[stage] + (late_base if stage else 0)
        return every.at[
            :,
            pl.ds(pl.multiple_of(start, BLOCK), size[stage]),
            pl.ds(pl.multiple_of(column * wide, wide), wide),
        ]

    def own_unit(stage):
        return own.at[:, pl.ds(early_rows if stage else 0, size[stage])]

    def await_unit(stage, owner, column, when=None):
        arrival(unit(stage, owner, column), r_unit.at[stage, owner, column], when)

    def to_sib(stage, slot, owner, column, when=None, source=None):
        here = unit(stage, owner, column)
        remote(
            here if source is None else source,
            here,
            s_sib.at[stage, slot, column],
            r_unit.at[stage, owner, column],
            at(base + q_sib),
            when,
        )

    def to_x(stage, owner, column, when=None, source=None):
        here = unit(stage, owner, column)
        remote(
            here if source is None else source,
            here,
            s_x.at[stage, column],
            r_unit.at[stage, owner, column],
            at(base + q_x),
            when,
        )

    def to_up(stage, slot, owner, column, when, source=None):
        here = unit(stage, owner, column)
        remote(
            here if source is None else source,
            here,
            s_up.at[stage, slot],
            r_unit.at[stage, owner, column],
            (r, c + 1),
            when,
        )

    def to_dn(stage, slot, owner, column, when, source=None):
        here = unit(stage, owner, column)
        remote(
            here if source is None else source,
            here,
            s_dn.at[stage, slot],
            r_unit.at[stage, owner, column],
            (r, c - 1),
            when,
        )

    low, high = c > 0, c + 1 < cols

    def first_step(stage):
        source = own_unit(stage)
        to_up(stage, 0, q, c, high, source)
        to_dn(stage, 0, q, c, low, source)
        to_x(stage, q, c, None, source)
        to_sib(stage, 0, q, c, None, source)

    def hop(stage, h):
        below, above = c - h, c + h
        ok_b, ok_a = below >= 0, above < cols
        await_unit(stage, q, below, ok_b)
        to_up(stage, h, q, below, ok_b & high)
        if h > 1:
            to_x(stage, q, below, ok_b)
        to_sib(stage, 0, q, below, ok_b)
        await_unit(stage, q, above, ok_a)
        to_dn(stage, h, q, above, ok_a & low)
        if h > 1:
            to_x(stage, q, above, ok_a)
        to_sib(stage, 0, q, above, ok_a)

    def take_x(stage):
        await_unit(stage, q_x, c)
        to_sib(stage, 1, q_x, c)

    def spread_x(stage):
        to_up(stage, cols, q_x, c, high)
        to_dn(stage, cols, q_x, c, low)

    def take_near(stage):
        await_unit(stage, q_x, c - 1, low)
        to_sib(stage, 1, q_x, c - 1, low)
        await_unit(stage, q_x, c + 1, high)
        to_sib(stage, 1, q_x, c + 1, high)

    def take_far(stage):
        for h in range(2, cols):
            await_unit(stage, q_x, c - h, c >= h)
            to_sib(stage, 1, q_x, c - h, c >= h)
            await_unit(stage, q_x, c + h, c + h < cols)
            to_sib(stage, 1, q_x, c + h, c + h < cols)

    def take_sib(stage):
        for owner in (q_sib, q_d):
            for column in range(cols):
                await_unit(stage, owner, column)

    shards = (gate_ref, up_ref, down_ref)

    def quarter(which, owner):
        return shards[which].at[:, pl.ds(pl.multiple_of(owner * fcol, fcol), fcol)]

    def w_rows(which, rank):
        return weights.at[which, pl.ds(pl.multiple_of(rank * drow, drow), drow)]

    def w_send(slot, which, source, rank, device):
        remote(source, w_rows(which, rank), s_w.at[slot, which], r_w.at[rank, which], device)

    def w_forward(slot, which, rank):
        arrival(w_rows(which, rank), r_w.at[rank, which])
        w_send(slot, which, w_rows(which, rank), rank, at(far + q))

    pl.semaphore_wait(barrier, ranks - 1 + as_int(low) + as_int(high))

    def box(owner):
        return outbox.at[pl.ds(owner * 2, 2)]

    remote(box(q), box(q), s_box.at[0], r_box.at[q], at(base + q_x))
    remote(box(q), box(q), s_box.at[1], r_box.at[q], at(base + q_sib))
    first_step(EARLY)
    local = []
    for which in range(3):
        w_send(0, which, quarter(which, q), r, at(far + q))
        w_send(1, which, quarter(which, q_sib), r, at(base + q_sib))
        copy = pltpu.make_async_copy(quarter(which, q), w_rows(which, r), s_loc.at[which])
        copy.start()
        local.append(copy)
    for which in range(3):
        w_send(2, which, quarter(which, q_x), r, at(base + q_x))
        w_send(3, which, quarter(which, q_d), r, at(base + q_d))
    tallies[r] = mine_ref[...]
    for step in range(1, ranks):
        remote(
            mine_ref,
            tallies.at[r],
            s_tally.at[step],
            r_tally.at[r],
            at(lax.rem(r + step, ranks)),
        )

    arrival(box(q_x), r_box.at[q_x])
    remote(box(q_x), box(q_x), s_box.at[2], r_box.at[q_x], at(base + q_sib))
    arrival(box(q_sib), r_box.at[q_sib])
    arrival(box(q_d), r_box.at[q_d])
    carry[...] = kept(outbox, pass_id, pass_ok)
    remote(carry, came, s_carry.at[0], r_carry.at[0], at(far + q))
    near = kept(outbox, near_id, near_ok)
    for which in range(3):
        w_forward(4, which, base + q_sib)
    hop(EARLY, 1)
    take_x(EARLY)
    arrival(came, r_carry.at[0])
    late_rows = pl.ds(pl.multiple_of(late_base + q * BLOCK, BLOCK), BLOCK)
    for which, ref in enumerate((tok_ref, grad_ref)):
        last = kept(ref, slot_id[WORK - 1], slot_ok[WORK - 1])
        last = jnp.where(far_ok > 0, came[which], jnp.where(near_ok > 0, near[which], last))
        own[which, early_rows : early_rows + BLOCK] = last
        every[which, late_rows, my_cols] = last
    first_step(LATE)
    hop(EARLY, 2)
    spread_x(EARLY)
    hop(LATE, 1)
    take_x(LATE)
    w_forward(5, 0, base + q_x)
    w_forward(6, 0, base + q_d)
    hop(EARLY, 3)
    hop(LATE, 2)
    spread_x(LATE)
    w_forward(5, 1, base + q_x)
    w_forward(6, 1, base + q_d)
    hop(LATE, 3)
    w_forward(5, 2, base + q_x)
    w_forward(6, 2, base + q_d)
    take_near(EARLY)
    take_far(EARLY)
    take_near(LATE)
    take_sib(EARLY)
    for copy in local:
        copy.wait()
    for which in range(3):
        for owner in range(group):
            arrival(w_rows(which, far + owner), r_w.at[far + owner, which])

    tile = 2 * BLOCK

    def forward_tile(index):
        rows = pl.ds(pl.multiple_of(index * tile, tile), tile)
        gate_sum = jnp.dot(every[0, rows], weights[0], preferred_element_type=jnp.float32)
        up_sum = jnp.dot(every[0, rows], weights[1], preferred_element_type=jnp.float32)
        back_sum = jnp.dot(every[1, rows], weights[2], preferred_element_type=jnp.float32)
        hidden, gate_back, up_back = local_terms(gate_sum, up_sum, back_sum)
        hid[rows] = hidden
        backs[rows, :fcol] = gate_back
        backs[rows, fcol:] = up_back

    early_tiles = late_base // tile
    all_tiles = every.shape[1] // tile
    pl.loop(0, early_tiles)(forward_tile)
    take_far(LATE)
    take_sib(LATE)
    pl.loop(early_tiles, all_tiles)(forward_tile)

    def hid_rows(stage, owner):
        start = owner * size[stage] + (late_base if stage else 0)
        return hid.at[pl.ds(pl.multiple_of(start, BLOCK), size[stage])]

    def hid_place(stage, owner):
        return hid_ref.at[
            pl.ds(early_rows if stage else 0, size[stage]),
            pl.ds(pl.multiple_of(owner * fcol, fcol), fcol),
        ]

    for stage in (EARLY, LATE):
        for slot, owner in enumerate((q_x, q_d, q_sib)):
            remote(
                hid_rows(stage, owner),
                hid_place(stage, q),
                s_hid.at[stage, slot],
                r_hid.at[stage, q],
                at(base + owner),
            )
        copy = pltpu.make_async_copy(
            hid_rows(stage, q), hid_place(stage, q), s_hid.at[stage, 3]
        )
        copy.start()
        local.append(copy)

    def turn(index):
        half = index // 2
        return ((x + 1 - half) % 2) * 2 + (k + index % 2 + half) % 2

    def grads_of(rank):
        wanted = pl.ds(pl.multiple_of(rank * drow, drow), drow)
        both = contract_rows(every[0, :, wanted], backs[...])
        return both[:, :fcol], both[:, fcol:], contract_rows(every[1, :, wanted], hid[...])

    def leave_copy(index):
        return pltpu.make_async_remote_copy(
            src_ref=leave.at[index],
            dst_ref=enter.at[index],
            send_sem=s_leave.at[index],
            recv_sem=r_leave.at[index],
            device_id=at(far + q),
            device_id_type=MESH,
        )

    def leave_tile(index):
        for which, value in enumerate(grads_of(far + turn(index))):
            leave[index, which] = value.astype(jnp.bfloat16)
        leave_copy(index).start()

    def stay_tile(index):
        for which, value in enumerate(grads_of(base + turn(index))):
            part[index, which] = value

    pl.loop(0, group)(leave_tile)
    pl.loop(0, group)(stay_tile)

    def sum_place(owner):
        return sum_ref.at[:, :, pl.ds(pl.multiple_of(owner * fcol, fcol), fcol)]

    for index, owner in enumerate((q_x, q_d, q_sib, q)):
        leave_copy(index).wait_recv()
        for which in range(3):
            final[index, which] = (
                part[index, which] + enter[index, which].astype(jnp.float32)
            ).astype(jnp.bfloat16)
        if index < group - 1:
            remote(
                final.at[index],
                sum_place(q),
                s_final.at[index],
                r_final.at[q],
                at(base + owner),
            )
        else:
            copy = pltpu.make_async_copy(final.at[index], sum_place(q), s_final.at[index])
            copy.start()
            local.append(copy)

    for step in range(1, ranks):
        peer = lax.rem(r + step, ranks)
        arrival(tallies.at[peer], r_tally.at[peer])
    total_ref[...] = jnp.sum(tallies[...], axis=0)
    for owner in (q_x, q_d, q_sib):
        for stage in (EARLY, LATE):
            arrival(hid_place(stage, owner), r_hid.at[stage, owner])
        arrival(sum_place(owner), r_final.at[owner])
    for copy in local[3:]:
        copy.wait()
    for index in range(group):
        leave_copy(index).wait_send()
    for when, copy in sends:
        if when is None:
            copy.wait_send()
        else:
            pl.when(when)(functools.partial(copy.wait_send))


def grouped_device(
    tokens, out_grad, counts, block_moves, segment_ids, gate_weight, up_weight, down_weight
):
    ranks = lax.axis_size("row")
    cols = lax.axis_size("col")
    me_rank = lax.axis_index("row")
    slot_rows, wide = tokens.shape
    cap = slot_rows // BLOCK
    drow, hidden_cols = gate_weight.shape
    group = ranks // 2
    fcol = hidden_cols // group
    work_rows = WORK * BLOCK
    features = cols * wide
    all_rows = group * work_rows
    my_count = counts[0]
    places = jnp.arange(slot_rows, dtype=jnp.int32)
    following = jnp.concatenate([segment_ids[1:], segment_ids[-1:]])
    own_weight = (places + 1 < my_count) & (following == segment_ids)
    masked = jnp.where(own_weight[:, None], out_grad, jnp.zeros_like(out_grad))
    tally = jnp.broadcast_to(jnp.sum(own_weight.astype(jnp.float32)), (8, 128))
    half = jnp.bfloat16
    dma = pltpu.SemaphoreType.DMA
    vmem = pl.BlockSpec(memory_space=pltpu.VMEM)
    smem = pl.BlockSpec(memory_space=pltpu.SMEM)
    anywhere = pl.BlockSpec(memory_space=pl.ANY)
    flops = 2 * 6 * all_rows * features * fcol
    hid_parts, grad_parts, totals = pl.pallas_call(
        functools.partial(grouped_kernel, ranks, cols, cap),
        out_shape=(
            jax.ShapeDtypeStruct((work_rows, hidden_cols), half),
            jax.ShapeDtypeStruct((3, drow, hidden_cols), half),
            jax.ShapeDtypeStruct((8, 128), jnp.float32),
        ),
        in_specs=[smem, smem, vmem, vmem, vmem, anywhere, anywhere, anywhere],
        out_specs=(anywhere, anywhere, vmem),
        scratch_shapes=[
            pltpu.VMEM((2, work_rows, wide), half),
            pltpu.VMEM((2, all_rows, features), half),
            pltpu.VMEM((3, features, fcol), half),
            pltpu.VMEM((all_rows, fcol), half),
            pltpu.VMEM((all_rows, 2 * fcol), half),
            pltpu.VMEM((group * 2, 2, BLOCK, wide), half),
            pltpu.VMEM((2, BLOCK, wide), half),
            pltpu.VMEM((2, BLOCK, wide), half),
            pltpu.VMEM((group, 3, drow, fcol), half),
            pltpu.VMEM((group, 3, drow, fcol), half),
            pltpu.VMEM((group, 3, drow, fcol), jnp.float32),
            pltpu.VMEM((group, 3, drow, fcol), half),
            pltpu.VMEM((ranks, 8, 128), jnp.float32),
            dma((2, group, cols)),
            dma((2, cols)),
            dma((2, cols + 1)),
            dma((2, cols + 1)),
            dma((2, 2, cols)),
            dma((ranks, 3)),
            dma((7, 3)),
            dma((3,)),
            dma((group,)),
            dma((3,)),
            dma((1,)),
            dma((1,)),
            dma((ranks,)),
            dma((ranks,)),
            dma((group,)),
            dma((group,)),
            dma((group,)),
            dma((group,)),
            dma((2, 4)),
            dma((2, group)),
        ],
        compiler_params=pltpu.CompilerParams(
            collective_id=0, has_side_effects=True, vmem_limit_bytes=62 * 2**20
        ),
        cost_estimate=pl.CostEstimate(
            flops=flops, bytes_accessed=32 * 2**20, transcendentals=all_rows * fcol
        ),
        name="grouped",
    )(
        counts,
        block_moves,
        tokens.reshape(cap, BLOCK, wide),
        masked.reshape(cap, BLOCK, wide),
        tally,
        gate_weight,
        up_weight,
        down_weight,
    )
    block_ids = jnp.arange(cap, dtype=jnp.int32)
    filled = (my_count + BLOCK - 1) // BLOCK
    gone = jnp.any(
        (block_moves[None, :, 0] == me_rank) & (block_moves[None, :, 2] == block_ids[:, None]),
        axis=1,
    )
    held = jnp.sum(((block_ids < filled) & jnp.logical_not(gone)).astype(jnp.int32))
    came = jnp.any(block_moves[:, 1] == me_rank)
    slots = jnp.arange(WORK, dtype=jnp.int32)
    last = WORK - 1
    swapped = jnp.where(slots == held, last, jnp.where(slots == last, held, slots))
    slots = jnp.where(came, swapped, slots)
    hidden = jnp.take(hid_parts.reshape(WORK, BLOCK, hidden_cols), slots, axis=0)
    hidden = hidden.reshape(work_rows, hidden_cols)
    sums = grad_parts.astype(jnp.float32) / totals[0, 0]
    return (hidden, sums[0], sums[1], sums[2])


def solution(mesh):
    placed = (
        P("row", "col"),
        P("row", "col"),
        P("row"),
        P(),
        P("row"),
        P("row", "col"),
        P("row", "col"),
        P("row", "col"),
    )
    body = grouped_device if mesh.shape["row"] == 8 else plain_device
    return jax.shard_map(
        body,
        mesh=mesh,
        in_specs=placed,
        out_specs=(P("row", "col"), P("row", "col"), P("row", "col"), P("row", "col")),
        check_vma=False,
    )
```

```python
import functools

import jax
import jax.numpy as jnp
from jax import lax
from jax.experimental import pallas as pl
from jax.experimental.pallas import tpu as pltpu
from jax.sharding import PartitionSpec as P

BLOCK = 128
WORK = 4
MESH = pl.DeviceIdType.MESH


def local_terms(gate_sum, up_sum, back_sum):
    logistic = jax.nn.sigmoid(gate_sum)
    activated = gate_sum * logistic
    hidden = (activated * up_sum).astype(jnp.bfloat16)
    gate_back = (back_sum * up_sum * logistic * (1.0 + gate_sum * (1.0 - logistic))).astype(
        jnp.bfloat16
    )
    up_back = (back_sum * activated).astype(jnp.bfloat16)
    return (hidden, gate_back, up_back)


def contract(left_side, right_side):
    return lax.dot_general(
        left_side, right_side, (((0,), (0,)), ((), ())), preferred_element_type=jnp.float32
    )


def ring_gather(piece):
    ranks = lax.axis_size("col")
    me = lax.axis_index("col")
    rows, cols = piece.shape
    shift = [(i, (i + 1) % ranks) for i in range(ranks)]
    whole = jnp.zeros((rows, ranks * cols), piece.dtype)
    whole = lax.dynamic_update_slice(whole, piece, (0, me * cols))
    for step in range(1, ranks):
        piece = lax.ppermute(piece, "col", shift)
        owner = (me - step + ranks) % ranks
        whole = lax.dynamic_update_slice(whole, piece, (0, owner * cols))
    return whole


def plain_device(
    tokens, out_grad, counts, block_moves, segment_ids, gate_weight, up_weight, down_weight
):
    ranks_all = lax.axis_size("row")
    me_rank = lax.axis_index("row")
    slot_rows = tokens.shape[0]
    cap_blocks = slot_rows // BLOCK
    feat_cols = tokens.shape[1]
    my_count = counts[0]
    places = jnp.arange(slot_rows, dtype=jnp.int32)
    following = jnp.concatenate([segment_ids[1:], segment_ids[-1:]])
    own_weight = ((places + 1 < my_count) & (following == segment_ids)).astype(jnp.float32)
    source = block_moves[:, 0]
    target = block_moves[:, 1]
    block_id = block_moves[:, 2]
    block_ids = jnp.arange(cap_blocks, dtype=jnp.int32)
    filled = (my_count + BLOCK - 1) // BLOCK
    moved_out = jnp.any(
        (source[None, :] == me_rank) & (block_id[None, :] == block_ids[:, None]), axis=1
    )
    kept_flag = (block_ids < filled) & jnp.logical_not(moved_out)
    arrive = target == me_rank
    flag_bits = jnp.concatenate([kept_flag, arrive]).astype(jnp.int32)
    local_ids = jnp.concatenate([block_ids, cap_blocks + source])
    list_place = jnp.cumsum(flag_bits) - 1
    slot_ids = jnp.arange(WORK, dtype=jnp.int32)
    slot_hit = (flag_bits[:, None] == 1) & (list_place[:, None] == slot_ids[None, :])
    slot_index = jnp.sum(jnp.where(slot_hit, local_ids[:, None] + 1, 0), axis=0) - 1
    peer_ids = jnp.arange(ranks_all, dtype=jnp.int32)
    outgoing = (source[None, :] == me_rank) & (target[None, :] == peer_ids[:, None])
    send_block = jnp.sum(jnp.where(outgoing, block_id[None, :], 0), axis=1)
    send_live = jnp.any(outgoing, axis=1)
    own_both = jnp.concatenate([tokens, out_grad], axis=1).reshape(cap_blocks, BLOCK, 2 * feat_cols)
    own_mask = own_weight.astype(jnp.bfloat16).reshape(cap_blocks, BLOCK)

    def outbox(block_rows):
        chosen = jnp.take(block_rows, send_block, axis=0)
        live_rows = send_live.reshape((-1,) + (1,) * (chosen.ndim - 1))
        return jnp.where(live_rows, chosen, jnp.zeros_like(chosen))

    whole_count = jnp.sum(own_weight).astype(jnp.int32)
    count_parts = jnp.broadcast_to(
        jnp.stack([whole_count // 256, whole_count % 256]).astype(jnp.bfloat16)[None, :],
        (ranks_all, 2),
    )
    got_both = lax.all_to_all(outbox(own_both), "row", split_axis=0, concat_axis=0, tiled=True)
    got_small = lax.all_to_all(
        jnp.concatenate([outbox(own_mask), count_parts], axis=1),
        "row",
        split_axis=0,
        concat_axis=0,
        tiled=True,
    )
    got_mask = got_small[:, :BLOCK]
    part_values = got_small[:, BLOCK:].astype(jnp.float32)
    loss_total = 256.0 * jnp.sum(part_values[:, 0]) + jnp.sum(part_values[:, 1])

    def to_work(pool_rows):
        chosen = jnp.take(pool_rows, jnp.maximum(slot_index, 0), axis=0)
        live_rows = (slot_index >= 0).reshape((-1,) + (1,) * (chosen.ndim - 1))
        return jnp.where(live_rows, chosen, jnp.zeros_like(chosen))

    work_both = to_work(jnp.concatenate([own_both, got_both])).reshape(WORK * BLOCK, 2 * feat_cols)
    work_mask = to_work(jnp.concatenate([own_mask, got_mask])).reshape(WORK * BLOCK)
    work_weight = work_mask.astype(jnp.float32)
    hidden_cols = gate_weight.shape[1]
    token_piece = work_both[:, :feat_cols]
    grad_piece = work_both[:, feat_cols:]
    full_tokens = ring_gather(token_piece)
    full_grad = ring_gather(grad_piece)
    gate_piece = lax.all_gather(gate_weight, "row", axis=0, tiled=True)
    up_piece = lax.all_gather(up_weight, "row", axis=0, tiled=True)
    down_piece = lax.all_gather(down_weight, "row", axis=0, tiled=True)
    gate_sum = jnp.dot(full_tokens, gate_piece, preferred_element_type=jnp.float32)
    up_sum = jnp.dot(full_tokens, up_piece, preferred_element_type=jnp.float32)
    back_raw = jnp.dot(full_grad, down_piece, preferred_element_type=jnp.float32)
    back_sum = back_raw * work_weight[:, None]
    hidden, gate_back, up_back = local_terms(gate_sum, up_sum, back_sum)
    weighted = full_grad * work_mask[:, None]

    def term_rows(left_side, right_side):
        return contract(left_side, right_side) / loss_total

    down_grad = lax.psum_scatter(
        term_rows(weighted, hidden).astype(jnp.bfloat16), "row", scatter_dimension=0, tiled=True
    ).astype(jnp.float32)
    other_part = lax.psum_scatter(
        jnp.concatenate(
            [term_rows(full_tokens, gate_back), term_rows(full_tokens, up_back)], axis=1
        ).astype(jnp.bfloat16),
        "row",
        scatter_dimension=0,
        tiled=True,
    ).astype(jnp.float32)
    gate_grad = other_part[:, :hidden_cols]
    up_grad = other_part[:, hidden_cols:]
    return (hidden, gate_grad, up_grad, down_grad)


EARLY, LATE = 0, 1


def contract_rows(left_side, right_side):
    return lax.dot_general(
        left_side, right_side, (((0,), (0,)), ((), ())), preferred_element_type=jnp.float32
    )


def grouped_kernel(
    ranks,
    cols,
    cap,
    count_ref,
    moves_ref,
    tok_ref,
    grad_ref,
    segment_ref,
    gate_ref,
    up_ref,
    down_ref,
    hid_ref,
    gate_out,
    up_out,
    down_out,
    total_ref,
    slots_ref,
    own,
    masked,
    mine,
    every,
    weights,
    hid,
    backs,
    outbox,
    carry,
    came,
    leave,
    enter,
    part,
    final,
    tallies,
    r_unit,
    s_x,
    s_up,
    s_dn,
    s_sib,
    r_w,
    s_w,
    s_loc,
    r_box,
    s_box,
    s_carry,
    r_carry,
    s_tally,
    r_tally,
    s_leave,
    r_leave,
    s_final,
    r_final,
    s_hid,
    r_hid,
):
    group = ranks // 2
    r = lax.axis_index("row")
    c = lax.axis_index("col")
    y = r // group
    q = r % group
    x = q // 2
    k = q % 2
    q_sib = x * 2 + 1 - k
    q_x = (1 - x) * 2 + k
    q_d = (1 - x) * 2 + 1 - k
    base = y * group
    far = (1 - y) * group
    wide = own.shape[2]
    drow = gate_ref.shape[0]
    fcol = weights.shape[2]
    early_rows = (WORK - 1) * BLOCK
    late_base = group * early_rows

    def at(row):
        return (row, c)

    barrier = pltpu.get_barrier_semaphore()
    for step in range(1, ranks):
        pl.semaphore_signal(
            barrier, inc=1, device_id=at(lax.rem(r + step, ranks)), device_id_type=MESH
        )

    @pl.when(c + 1 < cols)
    def _():
        pl.semaphore_signal(barrier, inc=1, device_id=(r, c + 1), device_id_type=MESH)

    @pl.when(c > 0)
    def _():
        pl.semaphore_signal(barrier, inc=1, device_id=(r, c - 1), device_id_type=MESH)

    moves = moves_ref.shape[0]
    src = [moves_ref[m, 0] for m in range(moves)]
    dst = [moves_ref[m, 1] for m in range(moves)]
    blk = [moves_ref[m, 2] for m in range(moves)]

    def as_int(flag):
        return jnp.where(flag, 1, 0)

    order = []
    for m in range(moves):
        before = jnp.int32(0)
        for e in range(m):
            before = before + as_int(src[e] == src[m])
        order.append(before)
    filled = (count_ref[0] + BLOCK - 1) // BLOCK
    slot_id = [jnp.int32(0)] * WORK
    slot_ok = [jnp.int32(0)] * WORK
    held = jnp.int32(0)
    for b in range(cap):
        gone = jnp.int32(0)
        for m in range(moves):
            gone = gone + as_int((src[m] == r) & (blk[m] == b))
        keep = as_int((b < filled) & (gone == 0))
        for s in range(WORK):
            hit = keep * as_int(held == s)
            slot_id[s] = slot_id[s] + b * hit
            slot_ok[s] = slot_ok[s] + hit
        held = held + keep
    box_id = [jnp.int32(0), jnp.int32(0)]
    box_ok = [jnp.int32(0), jnp.int32(0)]
    near_id = jnp.int32(0)
    near_ok = jnp.int32(0)
    far_ok = jnp.int32(0)
    pass_id = jnp.int32(0)
    pass_ok = jnp.int32(0)
    for m in range(moves):
        for j in range(2):
            hit = as_int((src[m] == r) & (order[m] == j))
            box_id[j] = box_id[j] + blk[m] * hit
            box_ok[j] = box_ok[j] + hit
        inside = as_int((src[m] % group) // 2 == x)
        place = ((src[m] // group) * 2 + src[m] % 2) * 2 + order[m]
        to_me = as_int(dst[m] == r)
        near_id = near_id + to_me * inside * place
        near_ok = near_ok + to_me * inside
        far_ok = far_ok + to_me * (1 - inside)
        over = as_int(dst[m] == base + q_x) * inside
        pass_id = pass_id + over * place
        pass_ok = pass_ok + over

    came_here = near_ok + far_ok
    for s in range(WORK):
        swapped = jnp.where(held == s, WORK - 1, s)
        if s == WORK - 1:
            swapped = jnp.minimum(held, WORK - 1)
        slots_ref[s] = jnp.where(came_here > 0, swapped, s)

    def kept(ref, index, ok):
        value = ref[index]
        return jnp.where(ok > 0, value, jnp.zeros_like(value))

    my_cols = pl.ds(pl.multiple_of(c * wide, wide), wide)

    def take_slots(which, ref):
        for s in range(WORK - 1):
            rows = pl.ds(pl.multiple_of(q * early_rows + s * BLOCK, BLOCK), BLOCK)
            value = kept(ref, slot_id[s], slot_ok[s])
            own[which, s * BLOCK : (s + 1) * BLOCK] = value
            every[which, rows, my_cols] = value

    take_slots(0, tok_ref)

    sends = []

    def remote(source, target, send_sem, recv_sem, device, when=None):
        copy = pltpu.make_async_remote_copy(
            src_ref=source,
            dst_ref=target,
            send_sem=send_sem,
            recv_sem=recv_sem,
            device_id=device,
            device_id_type=MESH,
        )
        sends.append((when, copy))
        if when is None:
            copy.start()
        else:
            pl.when(when)(lambda: copy.start())

    def arrival(target, recv_sem, when=None):
        copy = pltpu.make_async_remote_copy(
            src_ref=target,
            dst_ref=target,
            send_sem=s_tally.at[0],
            recv_sem=recv_sem,
            device_id=at(r),
            device_id_type=MESH,
        )
        if when is None:
            copy.wait_recv()
        else:
            pl.when(when)(lambda: copy.wait_recv())

    size = (early_rows, BLOCK)

    def unit(stage, which, owner, column):
        start = owner * size[stage] + (late_base if stage else 0)
        return every.at[
            which,
            pl.ds(pl.multiple_of(start, BLOCK), size[stage]),
            pl.ds(pl.multiple_of(column * wide, wide), wide),
        ]

    def own_unit(stage, which):
        return own.at[which, pl.ds(early_rows if stage else 0, size[stage])]

    def await_unit(stage, which, owner, column, when=None):
        arrival(
            unit(stage, which, owner, column), r_unit.at[stage, which, owner, column], when
        )

    def pass_on(send_sem, device, stage, which, owner, column, when=None, source=None):
        here = unit(stage, which, owner, column)
        remote(
            here if source is None else source,
            here,
            send_sem,
            r_unit.at[stage, which, owner, column],
            device,
            when,
        )

    def to_sib(stage, which, slot, *rest):
        pass_on(s_sib.at[stage, which, slot, rest[1]], at(base + q_sib), stage, which, *rest)

    def to_x(stage, which, *rest):
        pass_on(s_x.at[stage, which, rest[1]], at(base + q_x), stage, which, *rest)

    def to_up(stage, which, slot, *rest):
        pass_on(s_up.at[stage, which, slot], (r, c + 1), stage, which, *rest)

    def to_dn(stage, which, slot, *rest):
        pass_on(s_dn.at[stage, which, slot], (r, c - 1), stage, which, *rest)

    low, high = c > 0, c + 1 < cols
    middle = low & high
    outer = (c == 0) | (c + 1 == cols)

    def first_z(stage, which, up, dn):
        to_up(stage, which, 0, q, c, up, own_unit(stage, which))
        to_dn(stage, which, 0, q, c, dn, own_unit(stage, which))

    def first_x(stage, which):
        to_x(stage, which, q, c, None, own_unit(stage, which))

    def first_sib(stage, which):
        to_sib(stage, which, 0, q, c, None, own_unit(stage, which))

    def hop(stage, which, h, gate=None):
        for column, ok, onward, more in (
            (c - h, c >= h, to_up, high),
            (c + h, c + h < cols, to_dn, low),
        ):
            if gate is not None:
                ok = ok & gate
            await_unit(stage, which, q, column, ok)
            onward(stage, which, h, q, column, ok & more)
            if h > 2 or (h == 2 and (which == 1 or stage == LATE)):
                to_x(stage, which, q, column, ok)
            to_sib(stage, which, 0, q, column, ok)

    def take_x(stage, which, gate=None):
        await_unit(stage, which, q_x, c, gate)
        to_sib(stage, which, 1, q_x, c, gate)

    def spread_x(stage, which, up, dn):
        to_up(stage, which, cols, q_x, c, up)
        to_dn(stage, which, cols, q_x, c, dn)

    def take_near(stage, which):
        for column, ok, onward in ((c - 1, low, to_up), (c + 1, high, to_dn)):
            await_unit(stage, which, q_x, column, ok)
            if stage == EARLY and which == 0:
                onward(stage, which, cols + 1, q_x, column, middle)
            to_sib(stage, which, 1, q_x, column, ok)

    def take_far(stage, h):
        for which in (0, 1):
            for column, ok in ((c - h, c >= h), (c + h, c + h < cols)):
                await_unit(stage, which, q_x, column, ok)
                to_sib(stage, which, 1, q_x, column, ok)

    def take_sib(stage, column, when=None):
        for owner in (q_sib, q_d):
            for which in (0, 1):
                await_unit(stage, which, owner, column, when)

    shards = (gate_ref, up_ref, down_ref)

    def quarter(which, owner):
        return shards[which].at[:, pl.ds(pl.multiple_of(owner * fcol, fcol), fcol)]

    def w_rows(which, rank):
        return weights.at[which, pl.ds(pl.multiple_of(rank * drow, drow), drow)]

    def w_send(slot, which, source, rank, device):
        remote(source, w_rows(which, rank), s_w.at[slot, which], r_w.at[rank, which], device)

    def w_forward(slot, which, rank):
        arrival(w_rows(which, rank), r_w.at[rank, which])
        w_send(slot, which, w_rows(which, rank), rank, at(far + q))

    pl.semaphore_wait(barrier, ranks - 1 + as_int(low) + as_int(high))

    def box(owner):
        return outbox.at[pl.ds(owner * 2, 2)]

    b_own, b_sib = y * 2 + k, y * 2 + 1 - k
    b_far, b_diag = (1 - y) * 2 + k, (1 - y) * 2 + 1 - k
    first_z(EARLY, 0, high, low)
    first_x(EARLY, 0)
    first_sib(EARLY, 0)
    lane = lax.broadcasted_iota(jnp.int32, (1, BLOCK), 1)
    on_diagonal = lax.broadcasted_iota(jnp.int32, (BLOCK, BLOCK), 0) == lax.broadcasted_iota(
        jnp.int32, (BLOCK, BLOCK), 1
    )
    tally = jnp.zeros((1, BLOCK), jnp.float32)
    for b in range(cap):
        here = segment_ref[b : b + 1, :]
        after = segment_ref[min(b + 1, cap - 1) : min(b + 1, cap - 1) + 1, :]
        following = jnp.where(
            lane < BLOCK - 1,
            pltpu.roll(here, BLOCK - 1, axis=1),
            pltpu.roll(after, BLOCK - 1, axis=1),
        )
        weight = jnp.where(
            (lane + (b * BLOCK + 1) < count_ref[0]) & (following == here), 1.0, 0.0
        ).astype(jnp.float32)
        tally = tally + weight
        choose = jnp.where(on_diagonal, jnp.broadcast_to(weight, (BLOCK, BLOCK)), 0.0)
        masked[b] = jnp.dot(
            choose.astype(jnp.bfloat16), grad_ref[b], preferred_element_type=jnp.float32
        ).astype(jnp.bfloat16)
    mine[...] = jnp.broadcast_to(tally, mine.shape)


    take_slots(1, masked)
    first_z(EARLY, 1, high, low)
    first_x(EARLY, 1)
    first_sib(EARLY, 1)
    local = []

    def w_start(which):
        w_send(0, which, quarter(which, q), r, at(far + q))
        w_send(1, which, quarter(which, q_sib), r, at(base + q_sib))
        copy = pltpu.make_async_copy(quarter(which, q), w_rows(which, r), s_loc.at[which])
        copy.start()
        local.append(copy)

    def w_cross(which):
        w_send(2, which, quarter(which, q_x), r, at(base + q_x))
        w_send(3, which, quarter(which, q_d), r, at(base + q_d))

    def w_relay(which):
        w_forward(5, which, base + q_x)
        w_forward(6, which, base + q_d)

    w_start(0)
    for j in range(2):
        outbox[b_own * 2 + j, 0] = kept(tok_ref, box_id[j], box_ok[j])
        outbox[b_own * 2 + j, 1] = kept(masked, box_id[j], box_ok[j])
    tallies[r] = mine[...]
    remote(box(b_own), box(b_own), s_box.at[0], r_box.at[b_own], at(far + q))
    remote(box(b_own), box(b_own), s_box.at[1], r_box.at[b_own], at(base + q_sib))
    w_start(1)
    w_start(2)
    w_cross(0)
    for step in range(1, ranks):
        remote(
            mine, tallies.at[r], s_tally.at[step], r_tally.at[r], at(lax.rem(r + step, ranks))
        )

    hop(EARLY, 0, 1)
    take_x(EARLY, 0)
    hop(EARLY, 1, 1)
    spread_x(EARLY, 0, high, low)
    arrival(box(b_far), r_box.at[b_far])
    remote(box(b_far), box(b_far), s_box.at[2], r_box.at[b_far], at(base + q_sib))
    arrival(box(b_sib), r_box.at[b_sib])
    arrival(box(b_diag), r_box.at[b_diag])
    carry[...] = kept(outbox, pass_id, pass_ok)
    remote(carry, came, s_carry.at[0], r_carry.at[0], at(base + q_x))
    w_cross(1)
    w_cross(2)
    near = kept(outbox, near_id, near_ok)
    for which in range(3):
        w_forward(4, which, base + q_sib)
    take_x(EARLY, 1)
    hop(EARLY, 0, 2)
    w_relay(0)
    hop(EARLY, 1, 2)
    spread_x(EARLY, 1, high, low)
    arrival(came, r_carry.at[0])
    late_rows = pl.ds(pl.multiple_of(late_base + q * BLOCK, BLOCK), BLOCK)
    for which, ref in enumerate((tok_ref, masked)):
        last = kept(ref, slot_id[WORK - 1], slot_ok[WORK - 1])
        last = jnp.where(far_ok > 0, came[which], jnp.where(near_ok > 0, near[which], last))
        own[which, early_rows : early_rows + BLOCK] = last
        every[which, late_rows, my_cols] = last
    for which in (0, 1):
        first_sib(LATE, which)
        first_z(LATE, which, c == 0, c + 1 == cols)
    take_near(EARLY, 0)
    for which in (0, 1):
        first_z(LATE, which, middle, middle)
    w_relay(1)
    hop(EARLY, 0, 3)
    w_relay(2)
    hop(EARLY, 1, 3)
    for which in (0, 1):
        first_x(LATE, which)
    for which in (0, 1):
        hop(LATE, which, 1, middle)
    for which in (0, 1):
        hop(LATE, which, 2, middle)
    for which in (0, 1):
        take_x(LATE, which, middle)
        spread_x(LATE, which, middle, middle)
    take_near(EARLY, 1)
    for h in range(2, cols):
        take_far(EARLY, h)
    for column in range(cols):
        take_sib(EARLY, column)
    for copy in local:
        copy.wait()
    for which in range(3):
        for owner in range(group):
            arrival(w_rows(which, far + owner), r_w.at[far + owner, which])

    tile = 2 * BLOCK

    def keep_terms(rows, sums):
        hidden, gate_back, up_back = local_terms(*sums)
        hid[rows] = hidden
        backs[rows, :fcol] = gate_back
        backs[rows, fcol:] = up_back

    def tile_rows(index):
        return pl.ds(pl.multiple_of(index * tile, tile), tile)

    def forward_tile(index):
        rows = tile_rows(index)
        keep_terms(
            rows,
            [
                jnp.dot(
                    every[which // 2, rows], weights[which], preferred_element_type=jnp.float32
                )
                for which in range(3)
            ],
        )

    early_tiles = late_base // tile
    late_tiles = every.shape[1] // tile - early_tiles

    def late_column(column, opening):
        span = pl.ds(pl.multiple_of(column * wide, wide), wide)

        def one(index):
            rows = tile_rows(early_tiles + index)
            for which in range(3):
                value = jnp.dot(
                    every[which // 2, rows, span],
                    weights[which, span],
                    preferred_element_type=jnp.float32,
                )
                part[index, which] = value if opening else part[index, which] + value

        pl.loop(0, late_tiles)(one)

    def late_hop(h):
        for column, ok in ((c - h, c >= h), (c + h, c + h < cols)):
            take_sib(LATE, column, ok)
            pl.when(ok)(functools.partial(late_column, column, False))

    def late_close(index):
        keep_terms(tile_rows(early_tiles + index), [part[index, which] for which in range(3)])

    pl.loop(0, 1)(forward_tile)
    for which in (0, 1):
        hop(LATE, which, 1, outer)
    pl.loop(1, 2)(forward_tile)
    for which in (0, 1):
        take_x(LATE, which, outer)
        spread_x(LATE, which, c == 0, c + 1 == cols)
    for which in (0, 1):
        hop(LATE, which, 2, outer)
    pl.loop(2, 4)(forward_tile)
    for which in (0, 1):
        hop(LATE, which, 3)
    pl.loop(4, early_tiles)(forward_tile)
    take_sib(LATE, c)
    late_column(c, True)
    take_far(LATE, 2)
    late_hop(2)
    for which in (0, 1):
        take_near(LATE, which)
    for h in range(3, cols):
        take_far(LATE, h)
    late_hop(1)
    for h in range(3, cols):
        late_hop(h)
    pl.loop(0, late_tiles)(late_close)

    def hid_rows(stage, owner):
        start = owner * size[stage] + (late_base if stage else 0)
        return hid.at[pl.ds(pl.multiple_of(start, BLOCK), size[stage])]

    def hid_place(stage, owner):
        return hid_ref.at[
            pl.ds(early_rows if stage else 0, size[stage]),
            pl.ds(pl.multiple_of(owner * fcol, fcol), fcol),
        ]

    for stage in (EARLY, LATE):
        for slot, owner in enumerate((q_x, q_d, q_sib)):
            remote(
                hid_rows(stage, owner),
                hid_place(stage, q),
                s_hid.at[stage, slot],
                r_hid.at[stage, q],
                at(base + owner),
            )
        copy = pltpu.make_async_copy(
            hid_rows(stage, q), hid_place(stage, q), s_hid.at[stage, 3]
        )
        copy.start()
        local.append(copy)

    def turn(index):
        half = index // 2
        return ((x + 1 - half) % 2) * 2 + (k + index % 2 + half) % 2

    def down_of(rank):
        wanted = pl.ds(pl.multiple_of(rank * drow, drow), drow)
        return contract_rows(every[1, :, wanted], hid[...])

    def both_of(rank):
        wanted = pl.ds(pl.multiple_of(rank * drow, drow), drow)
        return contract_rows(every[0, :, wanted], backs[...])

    def leave_copy(index, first, count):
        return pltpu.make_async_remote_copy(
            src_ref=leave.at[index, pl.ds(first, count)],
            dst_ref=enter.at[index, pl.ds(first, count)],
            send_sem=s_leave.at[index, first],
            recv_sem=r_leave.at[index, first],
            device_id=at(far + q),
            device_id_type=MESH,
        )

    def leave_tile(index):
        rank = far + turn(index)
        leave[index, 0] = down_of(rank).astype(jnp.bfloat16)
        leave_copy(index, 0, 1).start()
        both = both_of(rank).astype(jnp.bfloat16)
        leave[index, 1] = both[:, :fcol]
        leave[index, 2] = both[:, fcol:]
        leave_copy(index, 1, 2).start()

    def stay_tile(index):
        rank = base + turn(index)
        part[index, 0] = down_of(rank)
        both = both_of(rank)
        part[index, 1] = both[:, :fcol]
        part[index, 2] = both[:, fcol:]

    pl.loop(0, group)(leave_tile)
    pl.loop(0, group)(stay_tile)

    outs = (down_out, gate_out, up_out)

    def sum_place(which, owner):
        return outs[which].at[:, pl.ds(pl.multiple_of(owner * fcol, fcol), fcol)]

    for index, owner in enumerate((q_x, q_d, q_sib, q)):
        for which in range(3):
            if which < 2:
                leave_copy(index, which, which + 1).wait_recv()
            final[index, which] = (
                part[index, which] + enter[index, which].astype(jnp.float32)
            ).astype(jnp.bfloat16)
        for which in range(3):
            if index < group - 1:
                remote(
                    final.at[index, which],
                    sum_place(which, q),
                    s_final.at[index, which],
                    r_final.at[q, which],
                    at(base + owner),
                )
            else:
                copy = pltpu.make_async_copy(
                    final.at[index, which], sum_place(which, q), s_final.at[index, which]
                )
                copy.start()
                local.append(copy)

    for step in range(1, ranks):
        peer = lax.rem(r + step, ranks)
        arrival(tallies.at[peer], r_tally.at[peer])
    total_ref[0] = jnp.sum(jnp.sum(tallies[...], axis=0)[:1])
    for owner in (q_x, q_d, q_sib):
        for stage in (EARLY, LATE):
            arrival(hid_place(stage, owner), r_hid.at[stage, owner])
        for which in range(3):
            arrival(sum_place(which, owner), r_final.at[owner, which])
    for copy in local[3:]:
        copy.wait()
    for index in range(group):
        for which in range(2):
            leave_copy(index, which, which + 1).wait_send()
    for when, copy in sends:
        if when is None:
            copy.wait_send()
        else:
            pl.when(when)(functools.partial(copy.wait_send))


PIECES = 4


def finish_kernel(
    slots_ref, total_ref, hid_ref, gate_ref, up_ref, down_ref, *rest
):
    outs, (hid_buf, taken, given, s_in, s_out) = rest[:4], rest[4:]
    sums = (gate_ref, up_ref, down_ref)
    rows = taken.shape[1] // PIECES
    scale = 1.0 / total_ref[0]

    def hid_in(s):
        return pltpu.make_async_copy(hid_ref.at[slots_ref[s]], hid_buf.at[s], s_in.at[3, s])

    def hid_out(s):
        return pltpu.make_async_copy(hid_buf.at[s], outs[0].at[s], s_out.at[3, s])

    def part_in(which, piece):
        cut = pl.ds(piece * rows, rows)
        return pltpu.make_async_copy(
            sums[which].at[cut], taken.at[which, cut], s_in.at[which, piece]
        )

    def part_out(which, piece):
        cut = pl.ds(piece * rows, rows)
        return pltpu.make_async_copy(
            given.at[which, cut], outs[1 + which].at[cut], s_out.at[which, piece]
        )

    grid = [(which, piece) for which in range(3) for piece in range(PIECES)]
    for which, piece in grid:
        part_in(which, piece).start()
    for s in range(WORK):
        hid_in(s).start()
    for which, piece in grid:
        part_in(which, piece).wait()
        cut = pl.ds(piece * rows, rows)
        given[which, cut] = taken[which, cut].astype(jnp.float32) * scale
        part_out(which, piece).start()
    for s in range(WORK):
        hid_in(s).wait()
        hid_out(s).start()
    for which, piece in grid:
        part_out(which, piece).wait()
    for s in range(WORK):
        hid_out(s).wait()


def finish(hid_parts, sums, total, slots):
    rows, width = hid_parts.shape
    drow = sums[0].shape[0]
    smem = pl.BlockSpec(memory_space=pltpu.SMEM)
    anywhere = pl.BlockSpec(memory_space=pl.ANY)
    grad = jax.ShapeDtypeStruct((drow, width), jnp.float32)
    blocks = (WORK, rows // WORK, width)
    outs = pl.pallas_call(
        finish_kernel,
        in_specs=[smem, smem] + [anywhere] * 4,
        out_specs=[anywhere] * 4,
        out_shape=(jax.ShapeDtypeStruct(blocks, hid_parts.dtype), grad, grad, grad),
        scratch_shapes=[
            pltpu.VMEM(blocks, hid_parts.dtype),
            pltpu.VMEM((3, drow, width), sums[0].dtype),
            pltpu.VMEM((3, drow, width), jnp.float32),
            pltpu.SemaphoreType.DMA((4, max(WORK, PIECES))),
            pltpu.SemaphoreType.DMA((4, max(WORK, PIECES))),
        ],
        name="finish",
    )(slots, total, hid_parts.reshape(blocks), *sums)
    return (outs[0].reshape(rows, width), *outs[1:])


def grouped_device(
    tokens, out_grad, counts, block_moves, segment_ids, gate_weight, up_weight, down_weight
):
    ranks = lax.axis_size("row")
    cols = lax.axis_size("col")
    slot_rows, wide = tokens.shape
    cap = slot_rows // BLOCK
    drow, hidden_cols = gate_weight.shape
    group = ranks // 2
    fcol = hidden_cols // group
    work_rows = WORK * BLOCK
    features = cols * wide
    all_rows = group * work_rows
    half = jnp.bfloat16
    dma = pltpu.SemaphoreType.DMA
    vmem = pl.BlockSpec(memory_space=pltpu.VMEM)
    smem = pl.BlockSpec(memory_space=pltpu.SMEM)
    anywhere = pl.BlockSpec(memory_space=pl.ANY)
    flops = 2 * 6 * all_rows * features * fcol
    hid_parts, gate_sum, up_sum, down_sum, total, slots = pl.pallas_call(
        functools.partial(grouped_kernel, ranks, cols, cap),
        out_shape=(
            jax.ShapeDtypeStruct((work_rows, hidden_cols), half),
            jax.ShapeDtypeStruct((drow, hidden_cols), half),
            jax.ShapeDtypeStruct((drow, hidden_cols), half),
            jax.ShapeDtypeStruct((drow, hidden_cols), half),
            jax.ShapeDtypeStruct((1,), jnp.float32),
            jax.ShapeDtypeStruct((WORK,), jnp.int32),
        ),
        in_specs=[smem, smem, vmem, vmem, vmem, anywhere, anywhere, anywhere],
        out_specs=(anywhere, anywhere, anywhere, anywhere, smem, smem),
        scratch_shapes=[
            pltpu.VMEM((2, work_rows, wide), half),
            pltpu.VMEM((cap, BLOCK, wide), half),
            pltpu.VMEM((8, BLOCK), jnp.float32),
            pltpu.VMEM((2, all_rows, features), half),
            pltpu.VMEM((3, features, fcol), half),
            pltpu.VMEM((all_rows, fcol), half),
            pltpu.VMEM((all_rows, 2 * fcol), half),
            pltpu.VMEM((group * 2, 2, BLOCK, wide), half),
            pltpu.VMEM((2, BLOCK, wide), half),
            pltpu.VMEM((2, BLOCK, wide), half),
            pltpu.VMEM((group, 3, drow, fcol), half),
            pltpu.VMEM((group, 3, drow, fcol), half),
            pltpu.VMEM((group, 3, drow, fcol), jnp.float32),
            pltpu.VMEM((group, 3, drow, fcol), half),
            pltpu.VMEM((ranks, 8, 128), jnp.float32),
            dma((2, 2, group, cols)),
            dma((2, 2, cols)),
            dma((2, 2, cols + 2)),
            dma((2, 2, cols + 2)),
            dma((2, 2, 2, cols)),
            dma((ranks, 3)),
            dma((7, 3)),
            dma((3,)),
            dma((group,)),
            dma((3,)),
            dma((1,)),
            dma((1,)),
            dma((ranks,)),
            dma((ranks,)),
            dma((group, 2)),
            dma((group, 2)),
            dma((group, 3)),
            dma((group, 3)),
            dma((2, 4)),
            dma((2, group)),
        ],
        compiler_params=pltpu.CompilerParams(
            collective_id=0, has_side_effects=True, vmem_limit_bytes=62 * 2**20
        ),
        cost_estimate=pl.CostEstimate(
            flops=flops, bytes_accessed=32 * 2**20, transcendentals=all_rows * fcol
        ),
        name="grouped",
    )(
        counts,
        block_moves,
        tokens.reshape(cap, BLOCK, wide),
        out_grad.reshape(cap, BLOCK, wide),
        segment_ids.reshape(cap, BLOCK),
        gate_weight,
        up_weight,
        down_weight,
    )
    return finish(hid_parts, (gate_sum, up_sum, down_sum), total, slots)


def solution(mesh):
    placed = (
        P("row", "col"),
        P("row", "col"),
        P("row"),
        P(),
        P("row"),
        P("row", "col"),
        P("row", "col"),
        P("row", "col"),
    )
    body = grouped_device if mesh.shape["row"] == 8 else plain_device
    return jax.shard_map(
        body,
        mesh=mesh,
        in_specs=placed,
        out_specs=(P("row", "col"), P("row", "col"), P("row", "col"), P("row", "col")),
        check_vma=False,
    )
```

```python
import functools

import jax
import jax.numpy as jnp
from jax import lax
from jax.experimental import pallas as pl
from jax.experimental.pallas import tpu as pltpu
from jax.sharding import PartitionSpec as P

BLOCK = 128
WORK = 4
MESH = pl.DeviceIdType.MESH


def local_terms(gate_sum, up_sum, back_sum):
    logistic = jax.nn.sigmoid(gate_sum)
    activated = gate_sum * logistic
    hidden = (activated * up_sum).astype(jnp.bfloat16)
    gate_back = (back_sum * up_sum * logistic * (1.0 + gate_sum * (1.0 - logistic))).astype(
        jnp.bfloat16
    )
    up_back = (back_sum * activated).astype(jnp.bfloat16)
    return (hidden, gate_back, up_back)


def contract(left_side, right_side):
    return lax.dot_general(
        left_side, right_side, (((0,), (0,)), ((), ())), preferred_element_type=jnp.float32
    )


def ring_gather(piece):
    ranks = lax.axis_size("col")
    me = lax.axis_index("col")
    rows, cols = piece.shape
    shift = [(i, (i + 1) % ranks) for i in range(ranks)]
    whole = jnp.zeros((rows, ranks * cols), piece.dtype)
    whole = lax.dynamic_update_slice(whole, piece, (0, me * cols))
    for step in range(1, ranks):
        piece = lax.ppermute(piece, "col", shift)
        owner = (me - step + ranks) % ranks
        whole = lax.dynamic_update_slice(whole, piece, (0, owner * cols))
    return whole


def plain_device(
    tokens, out_grad, counts, block_moves, segment_ids, gate_weight, up_weight, down_weight
):
    ranks_all = lax.axis_size("row")
    me_rank = lax.axis_index("row")
    slot_rows = tokens.shape[0]
    cap_blocks = slot_rows // BLOCK
    feat_cols = tokens.shape[1]
    my_count = counts[0]
    places = jnp.arange(slot_rows, dtype=jnp.int32)
    following = jnp.concatenate([segment_ids[1:], segment_ids[-1:]])
    own_weight = ((places + 1 < my_count) & (following == segment_ids)).astype(jnp.float32)
    source = block_moves[:, 0]
    target = block_moves[:, 1]
    block_id = block_moves[:, 2]
    block_ids = jnp.arange(cap_blocks, dtype=jnp.int32)
    filled = (my_count + BLOCK - 1) // BLOCK
    moved_out = jnp.any(
        (source[None, :] == me_rank) & (block_id[None, :] == block_ids[:, None]), axis=1
    )
    kept_flag = (block_ids < filled) & jnp.logical_not(moved_out)
    arrive = target == me_rank
    flag_bits = jnp.concatenate([kept_flag, arrive]).astype(jnp.int32)
    local_ids = jnp.concatenate([block_ids, cap_blocks + source])
    list_place = jnp.cumsum(flag_bits) - 1
    slot_ids = jnp.arange(WORK, dtype=jnp.int32)
    slot_hit = (flag_bits[:, None] == 1) & (list_place[:, None] == slot_ids[None, :])
    slot_index = jnp.sum(jnp.where(slot_hit, local_ids[:, None] + 1, 0), axis=0) - 1
    peer_ids = jnp.arange(ranks_all, dtype=jnp.int32)
    outgoing = (source[None, :] == me_rank) & (target[None, :] == peer_ids[:, None])
    send_block = jnp.sum(jnp.where(outgoing, block_id[None, :], 0), axis=1)
    send_live = jnp.any(outgoing, axis=1)
    own_both = jnp.concatenate([tokens, out_grad], axis=1).reshape(cap_blocks, BLOCK, 2 * feat_cols)
    own_mask = own_weight.astype(jnp.bfloat16).reshape(cap_blocks, BLOCK)

    def outbox(block_rows):
        chosen = jnp.take(block_rows, send_block, axis=0)
        live_rows = send_live.reshape((-1,) + (1,) * (chosen.ndim - 1))
        return jnp.where(live_rows, chosen, jnp.zeros_like(chosen))

    whole_count = jnp.sum(own_weight).astype(jnp.int32)
    count_parts = jnp.broadcast_to(
        jnp.stack([whole_count // 256, whole_count % 256]).astype(jnp.bfloat16)[None, :],
        (ranks_all, 2),
    )
    got_both = lax.all_to_all(outbox(own_both), "row", split_axis=0, concat_axis=0, tiled=True)
    got_small = lax.all_to_all(
        jnp.concatenate([outbox(own_mask), count_parts], axis=1),
        "row",
        split_axis=0,
        concat_axis=0,
        tiled=True,
    )
    got_mask = got_small[:, :BLOCK]
    part_values = got_small[:, BLOCK:].astype(jnp.float32)
    loss_total = 256.0 * jnp.sum(part_values[:, 0]) + jnp.sum(part_values[:, 1])

    def to_work(pool_rows):
        chosen = jnp.take(pool_rows, jnp.maximum(slot_index, 0), axis=0)
        live_rows = (slot_index >= 0).reshape((-1,) + (1,) * (chosen.ndim - 1))
        return jnp.where(live_rows, chosen, jnp.zeros_like(chosen))

    work_both = to_work(jnp.concatenate([own_both, got_both])).reshape(WORK * BLOCK, 2 * feat_cols)
    work_mask = to_work(jnp.concatenate([own_mask, got_mask])).reshape(WORK * BLOCK)
    work_weight = work_mask.astype(jnp.float32)
    hidden_cols = gate_weight.shape[1]
    token_piece = work_both[:, :feat_cols]
    grad_piece = work_both[:, feat_cols:]
    full_tokens = ring_gather(token_piece)
    full_grad = ring_gather(grad_piece)
    gate_piece = lax.all_gather(gate_weight, "row", axis=0, tiled=True)
    up_piece = lax.all_gather(up_weight, "row", axis=0, tiled=True)
    down_piece = lax.all_gather(down_weight, "row", axis=0, tiled=True)
    gate_sum = jnp.dot(full_tokens, gate_piece, preferred_element_type=jnp.float32)
    up_sum = jnp.dot(full_tokens, up_piece, preferred_element_type=jnp.float32)
    back_raw = jnp.dot(full_grad, down_piece, preferred_element_type=jnp.float32)
    back_sum = back_raw * work_weight[:, None]
    hidden, gate_back, up_back = local_terms(gate_sum, up_sum, back_sum)
    weighted = full_grad * work_mask[:, None]

    def term_rows(left_side, right_side):
        return contract(left_side, right_side) / loss_total

    down_grad = lax.psum_scatter(
        term_rows(weighted, hidden).astype(jnp.bfloat16), "row", scatter_dimension=0, tiled=True
    ).astype(jnp.float32)
    other_part = lax.psum_scatter(
        jnp.concatenate(
            [term_rows(full_tokens, gate_back), term_rows(full_tokens, up_back)], axis=1
        ).astype(jnp.bfloat16),
        "row",
        scatter_dimension=0,
        tiled=True,
    ).astype(jnp.float32)
    gate_grad = other_part[:, :hidden_cols]
    up_grad = other_part[:, hidden_cols:]
    return (hidden, gate_grad, up_grad, down_grad)


EARLY, LATE = 0, 1


def contract_rows(left_side, right_side):
    return lax.dot_general(
        left_side, right_side, (((0,), (0,)), ((), ())), preferred_element_type=jnp.float32
    )


def grouped_kernel(
    ranks,
    cols,
    cap,
    count_ref,
    moves_ref,
    tok_in,
    grad_in,
    segment_in,
    gate_ref,
    up_ref,
    down_ref,
    hid_ref,
    gate_out,
    up_out,
    down_out,
    total_ref,
    slots_ref,
    tok_ref,
    grad_ref,
    segment_ref,
    s_in,
    own,
    masked,
    mine,
    every,
    weights,
    hid,
    backs,
    outbox,
    carry,
    came,
    leave,
    enter,
    part,
    tallies,
    r_unit,
    s_x,
    s_up,
    s_dn,
    s_sib,
    r_w,
    s_w,
    s_loc,
    r_box,
    s_box,
    s_carry,
    r_carry,
    s_tally,
    r_tally,
    s_leave,
    r_leave,
    s_final,
    r_final,
    s_hid,
    r_hid,
):
    group = ranks // 2
    r = lax.axis_index("row")
    c = lax.axis_index("col")
    y = r // group
    q = r % group
    x = q // 2
    k = q % 2
    q_sib = x * 2 + 1 - k
    q_x = (1 - x) * 2 + k
    q_d = (1 - x) * 2 + 1 - k
    base = y * group
    far = (1 - y) * group
    wide = own.shape[2]
    drow = gate_ref.shape[0]
    fcol = weights.shape[2]
    early_rows = (WORK - 1) * BLOCK
    late_base = group * early_rows

    def at(row):
        return (row, c)

    loads = [
        pltpu.make_async_copy(source, target, s_in.at[index])
        for index, (source, target) in enumerate(
            ((tok_in, tok_ref), (segment_in, segment_ref), (grad_in, grad_ref))
        )
    ]
    for load in loads:
        load.start()
    barrier = pltpu.get_barrier_semaphore()
    for step in range(1, ranks):
        pl.semaphore_signal(
            barrier, inc=1, device_id=at(lax.rem(r + step, ranks)), device_id_type=MESH
        )

    @pl.when(c + 1 < cols)
    def _():
        pl.semaphore_signal(barrier, inc=1, device_id=(r, c + 1), device_id_type=MESH)

    @pl.when(c > 0)
    def _():
        pl.semaphore_signal(barrier, inc=1, device_id=(r, c - 1), device_id_type=MESH)

    moves = moves_ref.shape[0]
    src = [moves_ref[m, 0] for m in range(moves)]
    dst = [moves_ref[m, 1] for m in range(moves)]
    blk = [moves_ref[m, 2] for m in range(moves)]

    def as_int(flag):
        return jnp.where(flag, 1, 0)

    order = []
    for m in range(moves):
        before = jnp.int32(0)
        for e in range(m):
            before = before + as_int(src[e] == src[m])
        order.append(before)
    filled = (count_ref[0] + BLOCK - 1) // BLOCK
    slot_id = [jnp.int32(0)] * WORK
    slot_ok = [jnp.int32(0)] * WORK
    held = jnp.int32(0)
    for b in range(cap):
        gone = jnp.int32(0)
        for m in range(moves):
            gone = gone + as_int((src[m] == r) & (blk[m] == b))
        keep = as_int((b < filled) & (gone == 0))
        for s in range(WORK):
            hit = keep * as_int(held == s)
            slot_id[s] = slot_id[s] + b * hit
            slot_ok[s] = slot_ok[s] + hit
        held = held + keep
    box_id = [jnp.int32(0), jnp.int32(0)]
    box_ok = [jnp.int32(0), jnp.int32(0)]
    near_id = jnp.int32(0)
    near_ok = jnp.int32(0)
    far_ok = jnp.int32(0)
    pass_id = jnp.int32(0)
    pass_ok = jnp.int32(0)
    for m in range(moves):
        for j in range(2):
            hit = as_int((src[m] == r) & (order[m] == j))
            box_id[j] = box_id[j] + blk[m] * hit
            box_ok[j] = box_ok[j] + hit
        inside = as_int((src[m] % group) // 2 == x)
        place = ((src[m] // group) * 2 + src[m] % 2) * 2 + order[m]
        to_me = as_int(dst[m] == r)
        near_id = near_id + to_me * inside * place
        near_ok = near_ok + to_me * inside
        far_ok = far_ok + to_me * (1 - inside)
        over = as_int(dst[m] == base + q_x) * inside
        pass_id = pass_id + over * place
        pass_ok = pass_ok + over

    came_here = near_ok + far_ok
    for s in range(WORK):
        swapped = jnp.where(held == s, WORK - 1, s)
        if s == WORK - 1:
            swapped = jnp.minimum(held, WORK - 1)
        slots_ref[s] = jnp.where(came_here > 0, swapped, s)

    def kept(ref, index, ok):
        value = ref[index]
        return jnp.where(ok > 0, value, jnp.zeros_like(value))

    my_cols = pl.ds(pl.multiple_of(c * wide, wide), wide)

    def take_slots(which, ref):
        for s in range(WORK - 1):
            value = kept(ref, slot_id[s], slot_ok[s])
            own[which, s * BLOCK : (s + 1) * BLOCK] = value

    loads[0].wait()
    take_slots(0, tok_ref)

    sends = []

    def remote(source, target, send_sem, recv_sem, device, when=None):
        copy = pltpu.make_async_remote_copy(
            src_ref=source,
            dst_ref=target,
            send_sem=send_sem,
            recv_sem=recv_sem,
            device_id=device,
            device_id_type=MESH,
        )
        sends.append((when, copy))
        if when is None:
            copy.start()
        else:
            pl.when(when)(lambda: copy.start())

    def arrival(target, recv_sem, when=None):
        copy = pltpu.make_async_remote_copy(
            src_ref=target,
            dst_ref=target,
            send_sem=s_tally.at[0],
            recv_sem=recv_sem,
            device_id=at(r),
            device_id_type=MESH,
        )
        if when is None:
            copy.wait_recv()
        else:
            pl.when(when)(lambda: copy.wait_recv())

    size = (early_rows, BLOCK)

    def unit(stage, which, owner, column):
        start = owner * size[stage] + (late_base if stage else 0)
        return every.at[
            which,
            pl.ds(pl.multiple_of(start, BLOCK), size[stage]),
            pl.ds(pl.multiple_of(column * wide, wide), wide),
        ]

    def own_unit(stage, which):
        return own.at[which, pl.ds(early_rows if stage else 0, size[stage])]

    def await_unit(stage, which, owner, column, when=None):
        arrival(
            unit(stage, which, owner, column), r_unit.at[stage, which, owner, column], when
        )

    def pass_on(send_sem, device, stage, which, owner, column, when=None, source=None):
        here = unit(stage, which, owner, column)
        remote(
            here if source is None else source,
            here,
            send_sem,
            r_unit.at[stage, which, owner, column],
            device,
            when,
        )

    def to_sib(stage, which, slot, *rest):
        pass_on(s_sib.at[stage, which, slot, rest[1]], at(base + q_sib), stage, which, *rest)

    def to_x(stage, which, *rest):
        pass_on(s_x.at[stage, which, rest[1]], at(base + q_x), stage, which, *rest)

    def to_up(stage, which, slot, *rest):
        pass_on(s_up.at[stage, which, slot], (r, c + 1), stage, which, *rest)

    def to_dn(stage, which, slot, *rest):
        pass_on(s_dn.at[stage, which, slot], (r, c - 1), stage, which, *rest)

    low, high = c > 0, c + 1 < cols
    middle = low & high
    outer = (c == 0) | (c + 1 == cols)

    def first_z(stage, which, up, dn):
        to_up(stage, which, 0, q, c, up, own_unit(stage, which))
        to_dn(stage, which, 0, q, c, dn, own_unit(stage, which))

    def first_x(stage, which):
        to_x(stage, which, q, c, None, own_unit(stage, which))

    def first_sib(stage, which):
        to_sib(stage, which, 0, q, c, None, own_unit(stage, which))

    def hop(stage, which, h, gate=None):
        for column, ok, onward, more in (
            (c - h, c >= h, to_up, high),
            (c + h, c + h < cols, to_dn, low),
        ):
            if gate is not None:
                ok = ok & gate
            await_unit(stage, which, q, column, ok)
            onward(stage, which, h, q, column, ok & more)
            if h > 2 or (h == 2 and (which == 1 or stage == LATE)):
                to_x(stage, which, q, column, ok)
            to_sib(stage, which, 0, q, column, ok)

    def take_x(stage, which, gate=None):
        await_unit(stage, which, q_x, c, gate)
        to_sib(stage, which, 1, q_x, c, gate)

    def spread_x(stage, which, up, dn):
        to_up(stage, which, cols, q_x, c, up)
        to_dn(stage, which, cols, q_x, c, dn)

    def take_near(stage, which):
        for column, ok, onward in ((c - 1, low, to_up), (c + 1, high, to_dn)):
            await_unit(stage, which, q_x, column, ok)
            if stage == EARLY and which == 0:
                onward(stage, which, cols + 1, q_x, column, middle)
            to_sib(stage, which, 1, q_x, column, ok)

    def take_far(stage, h):
        for which in (0, 1):
            for column, ok in ((c - h, c >= h), (c + h, c + h < cols)):
                await_unit(stage, which, q_x, column, ok)
                to_sib(stage, which, 1, q_x, column, ok)

    def take_sib(stage, column, when=None):
        for owner in (q_sib, q_d):
            for which in (0, 1):
                await_unit(stage, which, owner, column, when)

    shards = (gate_ref, up_ref, down_ref)
    relayed = []

    def quarter(which, owner):
        return shards[which].at[:, pl.ds(pl.multiple_of(owner * fcol, fcol), fcol)]

    def w_rows(which, rank):
        return weights.at[which, pl.ds(pl.multiple_of(rank * drow, drow), drow)]

    def w_send(slot, which, source, rank, device):
        remote(source, w_rows(which, rank), s_w.at[slot, which], r_w.at[rank, which], device)

    def w_forward(slot, which, rank):
        arrival(w_rows(which, rank), r_w.at[rank, which])
        w_send(slot, which, w_rows(which, rank), rank, at(far + q))
        relayed.append(sends.pop()[1])

    pl.semaphore_wait(barrier, ranks - 1 + as_int(low) + as_int(high))

    def box(owner):
        return outbox.at[pl.ds(owner * 2, 2)]

    b_own, b_sib = y * 2 + k, y * 2 + 1 - k
    b_far, b_diag = (1 - y) * 2 + k, (1 - y) * 2 + 1 - k
    first_z(EARLY, 0, high, low)
    first_x(EARLY, 0)
    first_sib(EARLY, 0)
    loads[1].wait()
    loads[2].wait()
    lane = lax.broadcasted_iota(jnp.int32, (1, BLOCK), 1)
    on_diagonal = lax.broadcasted_iota(jnp.int32, (BLOCK, BLOCK), 0) == lax.broadcasted_iota(
        jnp.int32, (BLOCK, BLOCK), 1
    )
    tally = jnp.zeros((1, BLOCK), jnp.float32)
    for b in range(cap):
        here = segment_ref[b : b + 1, :]
        after = segment_ref[min(b + 1, cap - 1) : min(b + 1, cap - 1) + 1, :]
        following = jnp.where(
            lane < BLOCK - 1,
            pltpu.roll(here, BLOCK - 1, axis=1),
            pltpu.roll(after, BLOCK - 1, axis=1),
        )
        weight = jnp.where(
            (lane + (b * BLOCK + 1) < count_ref[0]) & (following == here), 1.0, 0.0
        ).astype(jnp.float32)
        tally = tally + weight
        choose = jnp.where(on_diagonal, jnp.broadcast_to(weight, (BLOCK, BLOCK)), 0.0)
        masked[b] = jnp.dot(
            choose.astype(jnp.bfloat16), grad_ref[b], preferred_element_type=jnp.float32
        ).astype(jnp.bfloat16)
    mine[...] = jnp.broadcast_to(tally, mine.shape)


    take_slots(1, masked)
    first_z(EARLY, 1, high, low)
    first_x(EARLY, 1)
    first_sib(EARLY, 1)
    local = []

    def w_start(which):
        w_send(0, which, quarter(which, q), r, at(far + q))
        w_send(1, which, quarter(which, q_sib), r, at(base + q_sib))
        copy = pltpu.make_async_copy(quarter(which, q), w_rows(which, r), s_loc.at[which])
        copy.start()
        local.append(copy)

    def w_cross(which):
        w_send(2, which, quarter(which, q_x), r, at(base + q_x))
        w_send(3, which, quarter(which, q_d), r, at(base + q_d))

    def w_relay(which):
        w_forward(5, which, base + q_x)
        w_forward(6, which, base + q_d)

    w_start(0)
    for j in range(2):
        outbox[b_own * 2 + j, 0] = kept(tok_ref, box_id[j], box_ok[j])
        outbox[b_own * 2 + j, 1] = kept(masked, box_id[j], box_ok[j])
    tallies[r] = mine[...]
    remote(box(b_own), box(b_own), s_box.at[0], r_box.at[b_own], at(far + q))
    remote(box(b_own), box(b_own), s_box.at[1], r_box.at[b_own], at(base + q_sib))
    w_start(1)
    w_start(2)
    w_cross(0)
    for step in range(1, ranks):
        remote(
            mine, tallies.at[r], s_tally.at[step], r_tally.at[r], at(lax.rem(r + step, ranks))
        )

    early_place = pl.ds(pl.multiple_of(q * early_rows, BLOCK), early_rows)
    for which in (0, 1):
        every[which, early_place, my_cols] = own[which, :early_rows]
    hop(EARLY, 0, 1)
    take_x(EARLY, 0)
    hop(EARLY, 1, 1)
    spread_x(EARLY, 0, high, low)
    arrival(box(b_far), r_box.at[b_far])
    remote(box(b_far), box(b_far), s_box.at[2], r_box.at[b_far], at(base + q_sib))
    arrival(box(b_sib), r_box.at[b_sib])
    arrival(box(b_diag), r_box.at[b_diag])
    carry[...] = kept(outbox, pass_id, pass_ok)
    remote(carry, came, s_carry.at[0], r_carry.at[0], at(base + q_x))
    w_cross(1)
    w_cross(2)
    near = kept(outbox, near_id, near_ok)
    for which in range(3):
        w_forward(4, which, base + q_sib)
    take_x(EARLY, 1)
    hop(EARLY, 0, 2)
    w_relay(0)
    hop(EARLY, 1, 2)
    spread_x(EARLY, 1, high, low)
    arrival(came, r_carry.at[0])
    late_rows = pl.ds(pl.multiple_of(late_base + q * BLOCK, BLOCK), BLOCK)
    for which, ref in enumerate((tok_ref, masked)):
        last = kept(ref, slot_id[WORK - 1], slot_ok[WORK - 1])
        last = jnp.where(far_ok > 0, came[which], jnp.where(near_ok > 0, near[which], last))
        own[which, early_rows : early_rows + BLOCK] = last
        every[which, late_rows, my_cols] = last
    for which in (0, 1):
        first_sib(LATE, which)
        first_z(LATE, which, c == 0, c + 1 == cols)
    take_near(EARLY, 0)
    for which in (0, 1):
        first_z(LATE, which, middle, middle)
    w_relay(1)
    hop(EARLY, 0, 3)
    w_relay(2)
    hop(EARLY, 1, 3)
    for which in (0, 1):
        first_x(LATE, which)
    for which in (0, 1):
        hop(LATE, which, 1, middle)
    for which in (0, 1):
        hop(LATE, which, 2, middle)
    for which in (0, 1):
        take_x(LATE, which, middle)
        spread_x(LATE, which, middle, middle)
    take_near(EARLY, 1)
    for h in range(2, cols):
        take_far(EARLY, h)
    for column in range(cols):
        take_sib(EARLY, column)
    for copy in local:
        copy.wait()
    for which in range(3):
        for owner in range(group):
            arrival(w_rows(which, far + owner), r_w.at[far + owner, which])

    tile = 2 * BLOCK

    def keep_terms(rows, sums):
        hidden, gate_back, up_back = local_terms(*sums)
        hid[rows] = hidden
        backs[rows, :fcol] = gate_back
        backs[rows, fcol:] = up_back

    def tile_rows(index):
        return pl.ds(pl.multiple_of(index * tile, tile), tile)

    def forward_tile(index):
        rows = tile_rows(index)
        keep_terms(
            rows,
            [
                jnp.dot(
                    every[which // 2, rows], weights[which], preferred_element_type=jnp.float32
                )
                for which in range(3)
            ],
        )

    early_tiles = late_base // tile
    late_tiles = every.shape[1] // tile - early_tiles

    def late_column(column, opening):
        span = pl.ds(pl.multiple_of(column * wide, wide), wide)

        def one(index):
            rows = tile_rows(early_tiles + index)
            for which in range(3):
                value = jnp.dot(
                    every[which // 2, rows, span],
                    weights[which, span],
                    preferred_element_type=jnp.float32,
                )
                part[index, which] = value if opening else part[index, which] + value

        pl.loop(0, late_tiles)(one)

    def late_hop(h):
        for column, ok in ((c - h, c >= h), (c + h, c + h < cols)):
            take_sib(LATE, column, ok)
            pl.when(ok)(functools.partial(late_column, column, False))

    def late_close(index):
        keep_terms(tile_rows(early_tiles + index), [part[index, which] for which in range(3)])

    pl.loop(0, 1)(forward_tile)
    for which in (0, 1):
        hop(LATE, which, 1, outer)
    pl.loop(1, 2)(forward_tile)
    for which in (0, 1):
        take_x(LATE, which, outer)
        spread_x(LATE, which, c == 0, c + 1 == cols)
    for which in (0, 1):
        hop(LATE, which, 2, outer)
    pl.loop(2, 4)(forward_tile)
    for which in (0, 1):
        hop(LATE, which, 3)
    pl.loop(4, early_tiles)(forward_tile)
    take_sib(LATE, c)
    late_column(c, True)
    take_far(LATE, 2)
    late_hop(2)
    for which in (0, 1):
        take_near(LATE, which)
    for h in range(3, cols):
        take_far(LATE, h)
    late_hop(1)
    for h in range(3, cols):
        late_hop(h)
    pl.loop(0, late_tiles)(late_close)

    def hid_rows(stage, owner):
        start = owner * size[stage] + (late_base if stage else 0)
        return hid.at[pl.ds(pl.multiple_of(start, BLOCK), size[stage])]

    def hid_place(stage, owner):
        return hid_ref.at[
            pl.ds(early_rows if stage else 0, size[stage]),
            pl.ds(pl.multiple_of(owner * fcol, fcol), fcol),
        ]

    for stage in (EARLY, LATE):
        for slot, owner in enumerate((q_x, q_d, q_sib)):
            remote(
                hid_rows(stage, owner),
                hid_place(stage, q),
                s_hid.at[stage, slot],
                r_hid.at[stage, q],
                at(base + owner),
            )
        copy = pltpu.make_async_copy(
            hid_rows(stage, q), hid_place(stage, q), s_hid.at[stage, 3]
        )
        copy.start()
        local.append(copy)

    def turn(index):
        half = index // 2
        return ((x + 1 - half) % 2) * 2 + (k + index % 2 + half) % 2

    def down_of(rank):
        wanted = pl.ds(pl.multiple_of(rank * drow, drow), drow)
        return contract_rows(every[1, :, wanted], hid[...])

    def both_of(rank):
        wanted = pl.ds(pl.multiple_of(rank * drow, drow), drow)
        return contract_rows(every[0, :, wanted], backs[...])

    def leave_copy(index, first, count):
        return pltpu.make_async_remote_copy(
            src_ref=leave.at[index, pl.ds(first, count)],
            dst_ref=enter.at[index, pl.ds(first, count)],
            send_sem=s_leave.at[index, first],
            recv_sem=r_leave.at[index, first],
            device_id=at(far + q),
            device_id_type=MESH,
        )

    def leave_tile(index):
        rank = far + turn(index)
        leave[index, 0] = down_of(rank).astype(jnp.bfloat16)
        leave_copy(index, 0, 1).start()
        both = both_of(rank).astype(jnp.bfloat16)
        leave[index, 1] = both[:, :fcol]
        leave[index, 2] = both[:, fcol:]
        leave_copy(index, 1, 2).start()

    def stay_tile(index):
        rank = base + turn(index)
        part[index, 0] = down_of(rank)
        both = both_of(rank)
        part[index, 1] = both[:, :fcol]
        part[index, 2] = both[:, fcol:]

    pl.loop(0, group)(leave_tile)
    pl.loop(0, group)(stay_tile)

    for copy in relayed:
        copy.wait_send()
    outs = (down_out, gate_out, up_out)

    def final(index, which):
        return weights.at[which, pl.ds(index * drow, drow)]

    def sum_place(which, owner):
        return outs[which].at[:, pl.ds(pl.multiple_of(owner * fcol, fcol), fcol)]

    for index, owner in enumerate((q_x, q_d, q_sib, q)):
        for which in range(3):
            if which < 2:
                leave_copy(index, which, which + 1).wait_recv()
            final(index, which)[...] = (
                part[index, which] + enter[index, which].astype(jnp.float32)
            ).astype(jnp.bfloat16)
        for which in range(3):
            if index < group - 1:
                remote(
                    final(index, which),
                    sum_place(which, q),
                    s_final.at[index, which],
                    r_final.at[q, which],
                    at(base + owner),
                )
            else:
                copy = pltpu.make_async_copy(
                    final(index, which), sum_place(which, q), s_final.at[index, which]
                )
                copy.start()
                local.append(copy)

    for step in range(1, ranks):
        peer = lax.rem(r + step, ranks)
        arrival(tallies.at[peer], r_tally.at[peer])
    total_ref[0] = jnp.sum(jnp.sum(tallies[...], axis=0)[:1])
    for owner in (q_x, q_d, q_sib):
        for stage in (EARLY, LATE):
            arrival(hid_place(stage, owner), r_hid.at[stage, owner])
        for which in range(3):
            arrival(sum_place(which, owner), r_final.at[owner, which])
    for copy in local[3:]:
        copy.wait()
    for index in range(group):
        for which in range(2):
            leave_copy(index, which, which + 1).wait_send()
    for when, copy in sends:
        if when is None:
            copy.wait_send()
        else:
            pl.when(when)(functools.partial(copy.wait_send))


PIECES = 4


def finish_kernel(
    slots_ref, total_ref, hid_ref, gate_ref, up_ref, down_ref, *rest
):
    outs, (hid_buf, taken, given, s_in, s_out) = rest[:4], rest[4:]
    sums = (gate_ref, up_ref, down_ref)
    rows = taken.shape[1] // PIECES
    scale = 1.0 / total_ref[0]

    def hid_in(s):
        return pltpu.make_async_copy(hid_ref.at[slots_ref[s]], hid_buf.at[s], s_in.at[3, s])

    def hid_out(s):
        return pltpu.make_async_copy(hid_buf.at[s], outs[0].at[s], s_out.at[3, s])

    def part_in(which, piece):
        cut = pl.ds(piece * rows, rows)
        return pltpu.make_async_copy(
            sums[which].at[cut], taken.at[which, cut], s_in.at[which, piece]
        )

    def part_out(which, piece):
        cut = pl.ds(piece * rows, rows)
        return pltpu.make_async_copy(
            given.at[which, cut], outs[1 + which].at[cut], s_out.at[which, piece]
        )

    grid = [(which, piece) for which in range(3) for piece in range(PIECES)]
    for which, piece in grid:
        part_in(which, piece).start()
    for s in range(WORK):
        hid_in(s).start()
    for which, piece in grid:
        part_in(which, piece).wait()
        cut = pl.ds(piece * rows, rows)
        given[which, cut] = taken[which, cut].astype(jnp.float32) * scale
        part_out(which, piece).start()
    for s in range(WORK):
        hid_in(s).wait()
        hid_out(s).start()
    for which, piece in grid:
        part_out(which, piece).wait()
    for s in range(WORK):
        hid_out(s).wait()


def finish(hid_parts, sums, total, slots):
    rows, width = hid_parts.shape
    drow = sums[0].shape[0]
    smem = pl.BlockSpec(memory_space=pltpu.SMEM)
    anywhere = pl.BlockSpec(memory_space=pl.ANY)
    grad = jax.ShapeDtypeStruct((drow, width), jnp.float32)
    blocks = (WORK, rows // WORK, width)
    outs = pl.pallas_call(
        finish_kernel,
        in_specs=[smem, smem] + [anywhere] * 4,
        out_specs=[anywhere] * 4,
        out_shape=(jax.ShapeDtypeStruct(blocks, hid_parts.dtype), grad, grad, grad),
        scratch_shapes=[
            pltpu.VMEM(blocks, hid_parts.dtype),
            pltpu.VMEM((3, drow, width), sums[0].dtype),
            pltpu.VMEM((3, drow, width), jnp.float32),
            pltpu.SemaphoreType.DMA((4, max(WORK, PIECES))),
            pltpu.SemaphoreType.DMA((4, max(WORK, PIECES))),
        ],
        name="finish",
    )(slots, total, hid_parts.reshape(blocks), *sums)
    return (outs[0].reshape(rows, width), *outs[1:])


def grouped_device(
    tokens, out_grad, counts, block_moves, segment_ids, gate_weight, up_weight, down_weight
):
    ranks = lax.axis_size("row")
    cols = lax.axis_size("col")
    slot_rows, wide = tokens.shape
    cap = slot_rows // BLOCK
    drow, hidden_cols = gate_weight.shape
    group = ranks // 2
    fcol = hidden_cols // group
    work_rows = WORK * BLOCK
    features = cols * wide
    all_rows = group * work_rows
    half = jnp.bfloat16
    dma = pltpu.SemaphoreType.DMA
    smem = pl.BlockSpec(memory_space=pltpu.SMEM)
    anywhere = pl.BlockSpec(memory_space=pl.ANY)
    flops = 2 * 6 * all_rows * features * fcol
    hid_parts, gate_sum, up_sum, down_sum, total, slots = pl.pallas_call(
        functools.partial(grouped_kernel, ranks, cols, cap),
        out_shape=(
            jax.ShapeDtypeStruct((work_rows, hidden_cols), half),
            jax.ShapeDtypeStruct((drow, hidden_cols), half),
            jax.ShapeDtypeStruct((drow, hidden_cols), half),
            jax.ShapeDtypeStruct((drow, hidden_cols), half),
            jax.ShapeDtypeStruct((1,), jnp.float32),
            jax.ShapeDtypeStruct((WORK,), jnp.int32),
        ),
        in_specs=[smem, smem] + [anywhere] * 6,
        out_specs=(anywhere, anywhere, anywhere, anywhere, smem, smem),
        scratch_shapes=[
            pltpu.VMEM((cap, BLOCK, wide), half),
            pltpu.VMEM((cap, BLOCK, wide), half),
            pltpu.VMEM((cap, BLOCK), jnp.int32),
            dma((3,)),
            pltpu.VMEM((2, work_rows, wide), half),
            pltpu.VMEM((cap, BLOCK, wide), half),
            pltpu.VMEM((8, BLOCK), jnp.float32),
            pltpu.VMEM((2, all_rows, features), half),
            pltpu.VMEM((3, features, fcol), half),
            pltpu.VMEM((all_rows, fcol), half),
            pltpu.VMEM((all_rows, 2 * fcol), half),
            pltpu.VMEM((group * 2, 2, BLOCK, wide), half),
            pltpu.VMEM((2, BLOCK, wide), half),
            pltpu.VMEM((2, BLOCK, wide), half),
            pltpu.VMEM((group, 3, drow, fcol), half),
            pltpu.VMEM((group, 3, drow, fcol), half),
            pltpu.VMEM((group, 3, drow, fcol), jnp.float32),
            pltpu.VMEM((ranks, 8, 128), jnp.float32),
            dma((2, 2, group, cols)),
            dma((2, 2, cols)),
            dma((2, 2, cols + 2)),
            dma((2, 2, cols + 2)),
            dma((2, 2, 2, cols)),
            dma((ranks, 3)),
            dma((7, 3)),
            dma((3,)),
            dma((group,)),
            dma((3,)),
            dma((1,)),
            dma((1,)),
            dma((ranks,)),
            dma((ranks,)),
            dma((group, 2)),
            dma((group, 2)),
            dma((group, 3)),
            dma((group, 3)),
            dma((2, 4)),
            dma((2, group)),
        ],
        compiler_params=pltpu.CompilerParams(
            collective_id=0, has_side_effects=True, vmem_limit_bytes=62 * 2**20
        ),
        cost_estimate=pl.CostEstimate(
            flops=flops, bytes_accessed=32 * 2**20, transcendentals=all_rows * fcol
        ),
        name="grouped",
    )(
        counts,
        block_moves,
        tokens.reshape(cap, BLOCK, wide),
        out_grad.reshape(cap, BLOCK, wide),
        segment_ids.reshape(cap, BLOCK),
        gate_weight,
        up_weight,
        down_weight,
    )
    return finish(hid_parts, (gate_sum, up_sum, down_sum), total, slots)


def solution(mesh):
    placed = (
        P("row", "col"),
        P("row", "col"),
        P("row"),
        P(),
        P("row"),
        P("row", "col"),
        P("row", "col"),
        P("row", "col"),
    )
    body = grouped_device if mesh.shape["row"] == 8 else plain_device
    return jax.shard_map(
        body,
        mesh=mesh,
        in_specs=placed,
        out_specs=(P("row", "col"), P("row", "col"), P("row", "col"), P("row", "col")),
        check_vma=False,
    )
```
